256 devices in a mesh: section: 16 (over y, z_lo, core), dp: 4 (over x), mp: 4 (over z_hi).
Axes of the slice: x: 4, y: 4, z: 8 (z_hi: 4, z_lo: 2; z = z_hi * 2 + z_lo), core: 2. Of those that a mesh axis runs over, the one named last changes fastest.
Arguments:
- patches: bfloat16 [32768, 1280], P(('section', 'dp')), may hold values from -6 to 6
- patch_counts: int32 [128], P(('section', 'dp')), may hold values from 8 to 256, as said below
- dest_rows: int32 [8192], P(('section', 'dp')), may hold values from 0 to 32767, as said below
- qkv_weight: bfloat16 [1280, 3, 1280], P(None, None, 'mp'), may hold values from -1 to 1
- out_weight: bfloat16 [1280, 1280], P('mp'), may hold values from -0.15625 to 0.15625
- attn_gain: bfloat16 [1280], replicated, may hold values from 0.25 to 1.75
- merge_gain: bfloat16 [1280], replicated, may hold values from 0.25 to 1.75
- fc1_weight: bfloat16 [5120, 5120], P('mp', ('section', 'dp')), may hold values from -0.078125 to 0.078125
- fc1_bias: bfloat16 [5120], P(('section', 'dp')), may hold values from -3 to 3
- fc2_weight: bfloat16 [5120, 8192], P(('section', 'dp'), 'mp'), may hold values from -0.078125 to 0.078125
- fc2_bias: bfloat16 [8192], P('mp'), may hold values from -3 to 3
- text_embeds: bfloat16 [32768, 8192], P(('section', 'dp'), 'mp'), may hold values from -6 to 6
- section_hidden: bfloat16 [32768, 8192], P(('section', 'dp'), 'mp'), may hold values from -80 to 80
- llm_gain: bfloat16 [8192], P('mp'), may hold values from 0.25 to 1.75
Outputs:
- sequence_embeds: bfloat16 [32768, 8192], P(('section', 'dp'), 'mp')
- layer_inputs: bfloat16 [32768, 8192], P(('section', 'dp'), 'mp')
The draws below stay inside these ranges and needn't reach their ends.
Inputs may be any that keep to these rules, and one draw needn't show every extreme that they name: `patch_counts`: multiples of 4; a tile's patches fill the first slots of its block. `dest_rows`: all rows differ. Each group's merged slots form runs of 2 consecutive slots (aligned); a run goes to one sequence slice (row // 512, numbered in section-major order), different runs of a group to different slices. Rows of slots that are not live are never written.
All inputs are finite; a program needn't handle non-finite values.
Results may differ from the reference program's by a relative error of at most 0.0055.
Values may be sent and summed in bfloat16 or wider, within the bound.
A program may use at most 128 MiB of HBM per device.

```python
import math
import jax
import jax.numpy as jnp
from jax import lax

D_VIT = 1280
HEADS = 16
HEAD_DIM = 80
MERGE_HID = 5120
HID = 8192
BLOCK = 256
TILES_DEV = 2
SEQ_ROWS = 512
GROUPS = 64
P_DEV = 512
M_DEV = 128
CAP = 2
PATCHES = 32768
TILES = 128
MERGE_IN = 5120
RECV_ROWS = 32768
N_SECTION = 16
N_DP = 4


def draw_patch_counts(key, part):
    return (4 * jax.random.randint(key, (TILES,), CAP, BLOCK // 4 + 1)).astype(jnp.int32)


def draw_dest_rows(key, part):
    group_total = GROUPS
    run_total = M_DEV // CAP
    heavy = jax.random.randint(jax.random.fold_in(key, 1), (), 0, group_total).astype(jnp.int32)

    def run_order(order_key):
        others = (heavy + 1 + jax.random.permutation(order_key, group_total - 1).astype(jnp.int32)) % group_total
        return jnp.concatenate([heavy[None], others])[:run_total]
    targets = jax.vmap(run_order)(jax.random.split(jax.random.fold_in(key, 2), group_total))
    places = jax.vmap(lambda place_key: jax.random.permutation(place_key, SEQ_ROWS).astype(jnp.int32))(jax.random.split(jax.random.fold_in(key, 3), group_total))
    source = jnp.arange(group_total, dtype=jnp.int32)[:, None, None]
    lane = jnp.arange(CAP, dtype=jnp.int32)[None, None, :]
    receiver = jnp.broadcast_to(targets[:, :, None], (group_total, run_total, CAP))
    position = places[receiver, source * CAP + lane]
    return (receiver * SEQ_ROWS + position).reshape(-1).astype(jnp.int32)


def draw_qkv_weight(key, part):
    base = jax.random.normal(key, (D_VIT, 3, D_VIT), jnp.float32) * D_VIT ** (-0.5)
    base = jnp.clip(base, -0.15, 0.15)
    return base.astype(jnp.bfloat16)


def draw_section_hidden(key, part):
    noise = jax.random.normal(jax.random.fold_in(key, 1), (RECV_ROWS, HID), jnp.float32)
    column_scale = jnp.exp(jnp.linspace(0.0, math.log(10.0), HID))[None, :]
    row_scale = jnp.exp(jax.random.uniform(jax.random.fold_in(key, 2), (RECV_ROWS, 1), jnp.float32, 0.0, math.log(10.0)))
    return jnp.clip(0.1 * noise * column_scale * row_scale, -80.0, 80.0).astype(jnp.bfloat16)


def shard_levels(key, shape, pieces, low, high):
    loudness = 1.0
    for axis_at, blocks in pieces:
        draws = jax.random.uniform(jax.random.fold_in(jax.random.fold_in(key, 6), axis_at), (blocks,), jnp.float32, low / len(pieces), high / len(pieces))
        loudness = loudness * jnp.repeat(jnp.exp(draws), shape[axis_at] // blocks).reshape((-1,) + (1,) * (len(shape) - 1 - axis_at))
    return loudness


def gaussian(own_key, dims, scale, bound, shards=(), kind=jnp.bfloat16):
    array = scale * jax.random.normal(own_key, dims, jnp.float32)
    if shards:
        array = array * shard_levels(own_key, dims, shards, -0.22, 0.18)
    return jnp.clip(array, -bound, bound).astype(kind)


def setup_inputs(seed: int = 0) -> dict:
    streams_of = jax.random.split(jax.random.key(seed), 15)
    return {
        "patches": gaussian(streams_of[0], (PATCHES, D_VIT), 1.0, 6.0, ((0, 64),)),
        "patch_counts": draw_patch_counts(jax.random.fold_in(streams_of[14], 71), 0),
        "dest_rows": draw_dest_rows(jax.random.fold_in(streams_of[14], 71), 0),
        "qkv_weight": draw_qkv_weight(jax.random.fold_in(streams_of[14], 71), 0),
        "out_weight": gaussian(streams_of[4], (D_VIT, D_VIT), D_VIT ** -0.5, 0.15625, ((0, 4),)),
        "attn_gain": jnp.clip(1.0 + 0.15 * jax.random.normal(streams_of[5], (D_VIT,), jnp.float32), 0.25, 1.75).astype(jnp.bfloat16),
        "merge_gain": jnp.clip(1.0 + 0.15 * jax.random.normal(streams_of[6], (D_VIT,), jnp.float32), 0.25, 1.75).astype(jnp.bfloat16),
        "fc1_weight": gaussian(streams_of[7], (MERGE_IN, MERGE_HID), MERGE_IN ** -0.5, 0.078125, ((0, 4), (1, 64))),
        "fc1_bias": gaussian(streams_of[8], (MERGE_HID,), 0.5, 3.0, ((0, 64),)),
        "fc2_weight": gaussian(streams_of[9], (MERGE_HID, HID), MERGE_HID ** -0.5, 0.078125, ((0, 64), (1, 4))),
        "fc2_bias": gaussian(streams_of[10], (HID,), 0.5, 3.0, ((0, 4),)),
        "text_embeds": gaussian(streams_of[11], (RECV_ROWS, HID), 1.0, 6.0, ((0, 64), (1, 4))),
        "section_hidden": draw_section_hidden(jax.random.fold_in(streams_of[14], 71), 0),
        "llm_gain": jnp.clip(1.0 + 0.15 * jax.random.normal(streams_of[13], (HID,), jnp.float32), 0.25, 1.75).astype(jnp.bfloat16),
    }


vit_eps = 1e-06
llm_eps = 1e-06

def layer_norm(values, gain):
    centred = values.astype(jnp.float32)
    centred = centred - lax.optimization_barrier(jnp.mean(centred, axis=-1, keepdims=True))
    variance = lax.optimization_barrier(jnp.mean(centred * centred, axis=-1, keepdims=True))
    return centred * lax.rsqrt(variance + vit_eps) * gain.astype(jnp.float32)

def group_embed(group_rows, group_counts, qkv_weight, out_weight, attn_gain, merge_gain, fc1_weight, fc1_bias, fc2_weight, fc2_bias):
    normed_in = layer_norm(group_rows, attn_gain).astype(jnp.bfloat16)
    projections = jnp.dot(normed_in, qkv_weight.reshape(D_VIT, 3 * D_VIT), preferred_element_type=jnp.float32).astype(jnp.bfloat16)
    projections = projections.reshape(TILES_DEV, BLOCK, 3, HEADS, HEAD_DIM).astype(jnp.float32)
    query_part = projections[:, :, 0]
    key_part = projections[:, :, 1]
    value_part = projections[:, :, 2]
    scores = jnp.einsum('tqhd,tkhd->thqk', query_part, key_part) * HEAD_DIM ** (-0.5)
    key_live = jnp.arange(BLOCK, dtype=jnp.int32)[None, None, None, :] < group_counts[:, None, None, None]
    scores = jnp.where(key_live, scores, -1e+30)
    weights = jax.nn.softmax(scores, axis=-1).astype(jnp.bfloat16)
    attended = jnp.einsum('thqk,tkhd->tqhd', weights.astype(jnp.float32), value_part).astype(jnp.bfloat16)
    attended = attended.reshape(P_DEV, D_VIT)
    block_out = (group_rows.astype(jnp.float32) + jnp.dot(attended, out_weight, preferred_element_type=jnp.float32)).astype(jnp.bfloat16)
    merge_in = layer_norm(block_out, merge_gain).astype(jnp.bfloat16).reshape(M_DEV, MERGE_IN)
    hidden = jax.nn.gelu(jnp.dot(merge_in, fc1_weight, preferred_element_type=jnp.float32) + fc1_bias.astype(jnp.float32), approximate=False).astype(jnp.bfloat16)
    return (jnp.dot(hidden, fc2_weight, preferred_element_type=jnp.float32) + fc2_bias.astype(jnp.float32)).astype(jnp.bfloat16)

def reference(patches, patch_counts, dest_rows, qkv_weight, out_weight, attn_gain, merge_gain, fc1_weight, fc1_bias, fc2_weight, fc2_bias, text_embeds, section_hidden, llm_gain):
    group_total = N_SECTION * N_DP
    grouped = patches.reshape(group_total, P_DEV, D_VIT)
    grouped_counts = patch_counts.reshape(group_total, TILES_DEV)

    def one_group(pair):
        return group_embed(pair[0], pair[1], qkv_weight, out_weight, attn_gain, merge_gain, fc1_weight, fc1_bias, fc2_weight, fc2_bias)
    image_embeds = lax.map(one_group, (grouped, grouped_counts)).reshape(group_total * M_DEV, HID)
    slot_in_tile = jnp.arange(group_total * M_DEV, dtype=jnp.int32) % (BLOCK // 4)
    tile_counts = jnp.repeat(patch_counts, BLOCK // 4, total_repeat_length=group_total * M_DEV)
    live = slot_in_tile * 4 < tile_counts
    target_rows = jnp.where(live, dest_rows, group_total * SEQ_ROWS).astype(jnp.int32)
    sequence_embeds = text_embeds.at[target_rows].set(image_embeds, mode='drop')
    sectioned_seq = sequence_embeds.reshape(N_SECTION, N_DP * SEQ_ROWS, HID)
    sectioned_hidden = section_hidden.reshape(N_SECTION, N_DP * SEQ_ROWS, HID)
    entering = jnp.concatenate([sectioned_seq[:1], sectioned_hidden[:-1]], axis=0).reshape(group_total * SEQ_ROWS, HID)
    entering = entering.astype(jnp.float32)
    mean_square = lax.optimization_barrier(jnp.mean(entering * entering, axis=1, keepdims=True))
    layer_inputs = (entering * lax.rsqrt(mean_square + llm_eps) * llm_gain.astype(jnp.float32)).astype(jnp.bfloat16)
    return (sequence_embeds, layer_inputs)
```

```python
import jax
import jax.numpy as jnp
from jax import lax
from jax.experimental import pallas as pl
from jax.experimental.pallas import tpu as pltpu
from jax.sharding import PartitionSpec as P

HEAD_DIM = 80
HID = 8192
MESH = pl.DeviceIdType.MESH
BF = jnp.bfloat16
F32 = jnp.float32

vit_eps = 1e-06
llm_eps = 1e-06


def place():
    s = lax.axis_index("section")
    x = lax.axis_index("dp")
    m = lax.axis_index("mp")
    return x, s // 4, (s // 2) % 2, s % 2, m


def at(x, y, zl, c, m):
    return (y * 4 + zl * 2 + c, x, m)


def greet(peers):
    barrier = pltpu.get_barrier_semaphore()
    for peer in peers:
        pl.semaphore_signal(barrier, inc=1, device_id=peer, device_id_type=MESH)
    pl.semaphore_wait(barrier, len(peers))


class Copies:
    def __init__(self, send, recv):
        self.send, self.recv, self.all = send, recv, []

    def go(self, src, dst, peer):
        k = len(self.all)
        copy = pltpu.make_async_remote_copy(
            src_ref=src,
            dst_ref=dst,
            send_sem=self.send.at[k],
            recv_sem=self.recv.at[k],
            device_id=peer,
            device_id_type=MESH,
        )
        copy.start()
        self.all.append(copy)
        return copy

    def drain(self):
        for copy in self.all:
            copy.wait_send()


def comm_call(body, ins, outs, copies, cid, limit=40 * 2**20):
    vm = pl.BlockSpec(memory_space=pltpu.VMEM)
    return pl.pallas_call(
        body,
        out_shape=[jax.ShapeDtypeStruct(s, d) for s, d in outs],
        in_specs=[vm] * len(ins),
        out_specs=[vm] * len(outs),
        scratch_shapes=[
            pltpu.SemaphoreType.DMA((copies,)),
            pltpu.SemaphoreType.DMA((copies,)),
        ],
        compiler_params=pltpu.CompilerParams(
            collective_id=cid, has_side_effects=True, vmem_limit_bytes=limit
        ),
    )(*ins)


def heads_kernel(part, fc2, dest, bias, rs, f2p, dall, ball, send, recv):
    x, y, zl, c, m = place()
    s = y * 4 + zl * 2 + c
    across = [(s, x, (m + k) % 4) for k in (2, 1, 3)]
    groups = [
        ((s + i) % 16, (x + j) % 4, m) for i in range(16) for j in range(4) if i or j
    ]
    greet(across + groups)
    cp = Copies(send, recv)
    for peer in across:
        cp.go(part.at[peer[2]], rs.at[m], peer)
    for dy in range(4):
        for dx in range(4):
            if dx or dy:
                px, py = (x + dx) % 4, (y + dy) % 4
                cols = pl.ds(pl.multiple_of((py * 4 + px) * 128, 128), 128)
                cp.go(fc2.at[:, cols], f2p.at[y * 4 + x], at(px, py, zl, c, m))
    for peer in groups:
        cp.go(dest, dall.at[s * 4 + x], peer)
    for dz in range(2):
        for dc in range(2):
            if dz or dc:
                cp.go(bias, ball.at[zl * 2 + c], at(x, y, (zl + dz) % 2, (c + dc) % 2, m))
    rs[m] = part[m]
    mine = y * 4 + x
    f2p[mine] = fc2[:, pl.ds(pl.multiple_of(mine * 128, 128), 128)]
    dall[s * 4 + x] = dest[...]
    ball[zl * 2 + c] = bias[...]
    for copy in cp.all:
        copy.wait_recv()
    cp.drain()


def gather_kernel(cut, blk, col, plane, column, send, recv):
    x, y, zl, c, m = place()
    z = 2 * m + zl
    xs = [(x + k) % 4 for k in range(4)]
    ys = [(y + k) % 4 for k in range(4)]
    zs = [(z + k) % 8 for k in range(8)]

    def zdev(zz, cc):
        return at(x, y, zz % 2, cc, zz // 2)

    right, left = at(xs[1], y, zl, c, m), at(xs[3], y, zl, c, m)
    up, down = at(x, ys[1], zl, c, m), at(x, ys[3], zl, c, m)
    above, below = zdev(zs[1], c), zdev(zs[7], c)
    twin = zdev(z, 1 - c)
    greet([right, left, up, down, above, below, twin])
    cp = Copies(send, recv)

    def block(v, a, b, lo, hi):
        fx, fy = (xs[a], ys[b]) if v == 0 else (xs[b], ys[a])
        return plane.at[2 * v + lo : 2 * v + hi, fy, fx]

    ahead = [[(right, left), (up, down)], [(up, down), (right, left)]]

    def push(v, axis, sgn, a, b, lo=0, hi=2, own=False):
        src = blk.at[2 * v + lo : 2 * v + hi] if own else block(v, a, b, lo, hi)
        return cp.go(src, block(v, a, b, lo, hi), ahead[v][axis][0 if sgn > 0 else 1])

    cpz = {}

    def hop(k):
        if k == 0:
            src = col
            cpz["u", 1] = cp.go(src, column.at[z, c], above)
            cpz["d", 1] = cp.go(src, column.at[z, c], below)
            cpz["t", 0] = cp.go(src, column.at[z, c], twin)
            return
        lo_, hi_ = zs[8 - k], zs[k]
        if k < 4:
            cpz["u", k].wait_recv()
            part = cut(0) if k == 3 else None
            ref = column.at[lo_, c]
            half = ref if part is None else ref.at[part]
            cpz["u", k + 1] = cp.go(half, half, above)
            cpz["t", k] = cp.go(ref, ref, twin)
            cpz["d", k].wait_recv()
            part = cut(1) if k == 3 else None
            ref = column.at[hi_, c]
            half = ref if part is None else ref.at[part]
            cpz["d", k + 1] = cp.go(half, half, below)
            cpz["t", -k] = cp.go(ref, ref, twin)
        else:
            cpz["u", 4].wait_recv()
            cpz["d", 4].wait_recv()
            ref = column.at[zs[4], c]
            cpz["t", 4] = cp.go(ref, ref, twin)

    hop(0)
    one, two, three, four = {}, {}, {}, {}
    for v in range(2):
        for g in (1, -1):
            one[v, g] = push(v, 0, g, 0, 0, own=True)
    for v in range(2):
        for g in (1, -1):
            three[v, 0, g] = push(v, 1, g, 0, 0, own=True)
    column[z, c] = col[...]
    plane[:, y, x] = blk[...]
    for g in (1, -1):
        for v in range(2):
            one[v, g].wait_recv()
            a = -g % 4
            two[v, g] = push(v, 0, g, a, 0, *((0, 1) if g > 0 else (1, 2)))
            for h in (1, -1):
                three[v, a, h] = push(v, 1, h, a, 0)
    hop(1)

    def opposite(a):
        for g in (1, -1):
            for v in range(2):
                three[v, a, g].wait_recv()
                four[v, a, g] = push(v, 1, g, a, -g % 4, *((0, 1) if g > 0 else (1, 2)))

    opposite(0)
    for v in range(2):
        for g in (1, -1):
            two[v, g].wait_recv()
        for h in (1, -1):
            three[v, 2, h] = push(v, 1, h, 2, 0)
    hop(2)
    opposite(3)
    opposite(1)
    hop(3)
    opposite(2)
    hop(4)
    for copy in four.values():
        copy.wait_recv()
    for key, copy in cpz.items():
        if key[0] == "t":
            copy.wait_recv()
    cp.drain()


def owner_kernel(out, emb, send, recv):
    x, y, zl, c, m = place()
    peers = [
        ((x + i) % 4, (y + j) % 4, (m + k) % 4)
        for i in range(4)
        for j in range(4)
        for k in range(4)
        if i or j or k
    ]
    greet([at(px, py, zl, c, pm) for px, py, pm in peers])
    cp = Copies(send, recv)
    mine = (pl.ds(pl.multiple_of(m * 32, 32), 32), pl.ds(pl.multiple_of((y * 4 + x) * 128, 128), 128))

    def rows(px, py):
        return pl.ds(pl.multiple_of((py * 4 + px) * 32, 32), 32)

    for px, py, pm in peers:
        cp.go(out.at[pm, rows(px, py)], emb.at[mine], at(px, py, zl, c, pm))
    emb[mine] = out[m, rows(x, y)]
    for copy in cp.all:
        copy.wait_recv()
    cp.drain()


def rows_kernel(rows, got, send, recv):
    s, d, m = lax.axis_index("section"), lax.axis_index("dp"), lax.axis_index("mp")
    peers = [((s + i) % 16, (d + j) % 4, m) for i in range(16) for j in range(4) if i or j]
    greet(peers)
    cp = Copies(send, recv)
    for peer in peers:
        cp.go(rows.at[peer[0] * 4 + peer[1]], got.at[s * 4 + d], peer)
    got[s * 4 + d] = rows[s * 4 + d]
    for copy in cp.all:
        copy.wait_recv()
    cp.drain()


def squares_kernel(own, every, send, recv):
    s, d, m = lax.axis_index("section"), lax.axis_index("dp"), lax.axis_index("mp")
    peers = [(s, d, (m + k) % 4) for k in (2, 1, 3)]
    greet(peers)
    cp = Copies(send, recv)
    for peer in peers:
        cp.go(own, every.at[m], peer)
    every[m] = own[...]
    for copy in cp.all:
        copy.wait_recv()
    cp.drain()


def layer_norm(values, gain):
    centred = values.astype(F32)
    centred = centred - jnp.mean(centred, axis=-1, keepdims=True)
    variance = jnp.mean(centred * centred, axis=-1, keepdims=True)
    return centred * lax.rsqrt(variance + vit_eps) * gain.astype(F32)


def per_device(
    patches,
    patch_counts,
    dest_rows,
    qkv_weight,
    out_weight,
    attn_gain,
    merge_gain,
    fc1_weight,
    fc1_bias,
    fc2_weight,
    fc2_bias,
    text_embeds,
    section_hidden,
    llm_gain,
):
    width = patches.shape[1]
    tiles, block = 2, 256
    local_cols = qkv_weight.shape[2]
    local_heads = local_cols // HEAD_DIM
    seq_rows = text_embeds.shape[0]
    merged = 128
    section, dp, mp = (lax.axis_index(a) for a in ("section", "dp", "mp"))
    incoming = lax.ppermute(section_hidden, "section", [(k, k + 1) for k in range(15)])

    normed_in = layer_norm(patches, attn_gain).astype(BF)
    projections = jnp.dot(
        normed_in, qkv_weight.reshape(width, 3 * local_cols), preferred_element_type=F32
    ).astype(BF)
    projections = projections.reshape(tiles, block, 3, local_heads, HEAD_DIM)
    query_part, key_part, value_part = (projections[:, :, k] for k in range(3))
    scores = jnp.einsum(
        "tqhd,tkhd->thqk", query_part, key_part, preferred_element_type=F32
    ) * HEAD_DIM ** (-0.5)
    key_live = jnp.arange(block, dtype=jnp.int32)[None, None, None, :] < patch_counts[:, None, None, None]
    scores = jnp.where(key_live, scores, -1e30)
    weights = jax.nn.softmax(scores, axis=-1).astype(BF)
    attended = jnp.einsum(
        "thqk,tkhd->tqhd", weights, value_part, preferred_element_type=F32
    ).astype(BF)
    attended = attended.reshape(patches.shape[0], local_cols)
    partial_proj = jnp.dot(attended, out_weight, preferred_element_type=F32).astype(BF)

    slot_in_tile = jnp.arange(merged, dtype=jnp.int32) % (block // 4)
    tile_counts = jnp.repeat(patch_counts, block // 4, total_repeat_length=merged)
    live = slot_in_tile * 4 < tile_counts
    dest_live = jnp.where(live, dest_rows, 2**30)[None, :]
    rs, f2p, dall, ball = comm_call(
        heads_kernel,
        (
            partial_proj.reshape(4, 128, width),
            fc2_weight,
            dest_live,
            jnp.broadcast_to(fc1_bias[:, None], (80, 128)),
        ),
        [
            ((4, 128, width), BF),
            ((16, 80, 128), BF),
            ((64, 1, 128), jnp.int32),
            ((4, 80, 128), BF),
        ],
        3 + 15 + 63 + 3,
        1,
    )
    own_patches = lax.dynamic_slice_in_dim(patches, mp * 128, 128, 0)
    block_out = (own_patches.astype(F32) + rs.astype(F32).sum(0)).astype(BF)
    merge_part = layer_norm(block_out, merge_gain).astype(BF)
    merge_part = merge_part.reshape(32, 4, width).transpose(1, 0, 2)

    rows_all, fc1_all = comm_call(
        lambda *a: gather_kernel(
            lambda k: (slice(None), slice(640 * k, 640 * (k + 1))), *a
        ),
        (merge_part, fc1_weight.T),
        [((4, 4, 4, 32, width), BF), ((8, 2, 80, width), BF)],
        40 + 16,
        2,
    )
    rows_all = rows_all.reshape(4, 512, width)
    fc1_all = fc1_all.reshape(4, 320, width)
    first = sum(
        lax.dot_general(
            fc1_all[p], rows_all[p], (((1,), (1,)), ((), ())), preferred_element_type=F32
        )
        for p in range(4)
    )
    first = first + ball.reshape(320, 128)[:, :1].astype(F32)
    hidden = jax.nn.gelu(first, approximate=False).astype(BF)

    hidden_all, fc2_all = comm_call(
        lambda *a: gather_kernel(lambda k: (slice(8 * k, 8 * (k + 1)),), *a),
        (hidden.reshape(4, 80, 512), f2p),
        [((4, 4, 4, 80, 512), BF), ((8, 2, 16, 80, 128), BF)],
        40 + 16,
        3,
    )
    hidden_all = hidden_all.reshape(5120, 512)
    fc2_all = fc2_all.reshape(4, 5120, 128)
    second = jnp.stack(
        [
            lax.dot_general(
                hidden_all, fc2_all[k], (((0,), (0,)), ((), ())), preferred_element_type=F32
            ).astype(BF)
            for k in range(4)
        ]
    )
    (embeds,) = comm_call(owner_kernel, (second,), [((128, 2048), BF)], 63, 4)
    embeds = (embeds.astype(F32) + fc2_bias.astype(F32)).astype(BF)

    slot = (dest_rows // seq_rows) * 2 + jnp.arange(merged, dtype=jnp.int32) % 2
    pick = (jnp.arange(merged, dtype=jnp.int32)[:, None] == slot[None, :]).astype(BF)
    send_rows = jnp.dot(pick, embeds, preferred_element_type=F32).astype(BF)
    (got,) = comm_call(
        rows_kernel, (send_rows.reshape(64, 2, 2048),), [((64, 2, 2048), BF)], 63, 5
    )
    own_slice = section * 4 + dp
    dall = dall.reshape(64, 64, 2)
    spots = jnp.where(dall // seq_rows == own_slice, dall % seq_rows, -1).max(axis=1).reshape(128)
    put = jnp.arange(seq_rows, dtype=jnp.int32)[:, None] == spots[None, :]
    hit = jnp.any(put, axis=1, keepdims=True)
    placed = jnp.dot(put.astype(BF), got.reshape(128, 2048), preferred_element_type=F32).astype(BF)
    sequence_embeds = jnp.where(hit, placed, text_embeds)
    entering = jnp.where(section == 0, sequence_embeds, incoming).astype(F32)
    squares = jnp.sum(entering * entering, axis=1)
    (every,) = comm_call(squares_kernel, (squares.reshape(4, 128),), [((4, 4, 128), F32)], 3, 6)
    row_total = every.sum(axis=0).reshape(seq_rows)
    layer_inputs = (
        entering * lax.rsqrt(row_total / HID + llm_eps)[:, None] * llm_gain.astype(F32)
    ).astype(BF)
    return (sequence_embeds, layer_inputs)


def solution(mesh):
    in_specs = (
        P(("section", "dp"), None),
        P(("section", "dp")),
        P(("section", "dp")),
        P(None, None, "mp"),
        P("mp", None),
        P(),
        P(),
        P("mp", ("section", "dp")),
        P(("section", "dp")),
        P(("section", "dp"), "mp"),
        P("mp"),
        P(("section", "dp"), "mp"),
        P(("section", "dp"), "mp"),
        P("mp"),
    )
    out_specs = (P(("section", "dp"), "mp"), P(("section", "dp"), "mp"))
    return jax.shard_map(
        per_device, mesh=mesh, in_specs=in_specs, out_specs=out_specs, check_vma=False
    )
```

```python
import jax
import jax.numpy as jnp
from jax import lax
from jax.experimental import pallas as pl
from jax.experimental.pallas import tpu as pltpu
from jax.sharding import PartitionSpec as P

HEAD_DIM = 80
HID = 8192
MESH = pl.DeviceIdType.MESH
BF = jnp.bfloat16
F32 = jnp.float32

vit_eps = 1e-06
llm_eps = 1e-06


def place():
    s = lax.axis_index("section")
    x = lax.axis_index("dp")
    m = lax.axis_index("mp")
    return x, s // 4, (s // 2) % 2, s % 2, m


def at(x, y, zl, c, m):
    return (y * 4 + zl * 2 + c, x, m)


def greet(peers):
    barrier = pltpu.get_barrier_semaphore()
    for peer in peers:
        pl.semaphore_signal(barrier, inc=1, device_id=peer, device_id_type=MESH)
    pl.semaphore_wait(barrier, len(peers))


class Copies:
    def __init__(self, send, recv):
        self.send, self.recv, self.all = send, recv, []

    def go(self, src, dst, peer):
        k = len(self.all)
        copy = pltpu.make_async_remote_copy(
            src_ref=src,
            dst_ref=dst,
            send_sem=self.send.at[k],
            recv_sem=self.recv.at[k],
            device_id=peer,
            device_id_type=MESH,
        )
        copy.start()
        self.all.append(copy)
        return copy

    def drain(self):
        for copy in self.all:
            copy.wait_send()


def column_gather(cp, cut, col, column, pos):
    x, y, zl, c, m = pos
    z = 2 * m + zl
    zs = [(z + k) % 8 for k in range(8)]

    def zdev(zz, cc):
        return at(x, y, zz % 2, cc, zz // 2)

    above, below, twin = zdev(zs[1], c), zdev(zs[7], c), zdev(z, 1 - c)
    up, down, side = {}, {}, []

    def hop(k):
        if k == 0:
            up[1] = cp.go(col, column.at[z, c], above)
            down[1] = cp.go(col, column.at[z, c], below)
            side.append(cp.go(col, column.at[z, c], twin))
        elif k < 4:
            for ways, z_from, peer, part in ((up, zs[8 - k], above, 0), (down, zs[k], below, 1)):
                ways[k].wait_recv()
                ref = column.at[z_from, c]
                half = ref.at[cut(part)] if k == 3 else ref
                ways[k + 1] = cp.go(half, half, peer)
                side.append(cp.go(ref, ref, twin))
        else:
            up[4].wait_recv()
            down[4].wait_recv()
            ref = column.at[zs[4], c]
            side.append(cp.go(ref, ref, twin))

    def finish():
        for copy in side:
            copy.wait_recv()

    return hop, finish


def plane_gather(cp, blk, plane, hop, pos):
    x, y, zl, c, m = pos
    xs = [(x + k) % 4 for k in range(4)]
    ys = [(y + k) % 4 for k in range(4)]
    right, left = at(xs[1], y, zl, c, m), at(xs[3], y, zl, c, m)
    up, down = at(x, ys[1], zl, c, m), at(x, ys[3], zl, c, m)
    ahead = [[(right, left), (up, down)], [(up, down), (right, left)]]

    def block(v, a, b, lo, hi):
        fx, fy = (xs[a], ys[b]) if v == 0 else (xs[b], ys[a])
        return plane.at[2 * v + lo : 2 * v + hi, fy, fx]

    def push(v, axis, sgn, a, b, lo=0, hi=2, own=False):
        src = blk.at[2 * v + lo : 2 * v + hi] if own else block(v, a, b, lo, hi)
        return cp.go(src, block(v, a, b, lo, hi), ahead[v][axis][0 if sgn > 0 else 1])

    one, two, three, four = {}, {}, {}, {}
    for v in range(2):
        for g in (1, -1):
            one[v, g] = push(v, 0, g, 0, 0, own=True)
    for v in range(2):
        for g in (1, -1):
            three[v, 0, g] = push(v, 1, g, 0, 0, own=True)
    hop(0)
    plane[:, y, x] = blk[...]
    for g in (1, -1):
        for v in range(2):
            one[v, g].wait_recv()
            a = -g % 4
            two[v, g] = push(v, 0, g, a, 0, *((0, 1) if g > 0 else (1, 2)))
            for h in (1, -1):
                three[v, a, h] = push(v, 1, h, a, 0)
    hop(1)

    def opposite(a):
        for g in (1, -1):
            for v in range(2):
                three[v, a, g].wait_recv()
                four[v, a, g] = push(v, 1, g, a, -g % 4, *((0, 1) if g > 0 else (1, 2)))

    opposite(0)
    for v in range(2):
        for g in (1, -1):
            two[v, g].wait_recv()
        for h in (1, -1):
            three[v, 2, h] = push(v, 1, h, 2, 0)
    hop(2)
    opposite(3)
    opposite(1)
    hop(3)
    opposite(2)
    hop(4)
    for copy in four.values():
        copy.wait_recv()


NT = (((1,), (1,)), ((), ()))
TN = (((0,), (0,)), ((), ()))


def dot(a, b, dims=(((1,), (0,)), ((), ()))):
    return lax.dot_general(a, b, dims, preferred_element_type=F32)


def normed(v, gain):
    v = v - jnp.mean(v, axis=-1, keepdims=True)
    return v * lax.rsqrt(jnp.mean(v * v, axis=-1, keepdims=True) + vit_eps) * gain


def step_kernel(
    patches, key_bias, wqkv, wout, attn_gain, merge_gain, fc1, fc1_bias, fc2, fc2_bias,
    dest, pick, llm_gain, text_hbm, hidden_hbm,
    seq_out, layer_out,
    text, incoming, xn, att, attr, wout_all, f2p, dall, ball, nrm, turn, blk1, rows_all, fc1_all,
    blk2, hid_all, fc2_all, acc, second, emb, flat, send_rows, got, sq_own, sq_all,
    send, recv, send3, recv3, local, relay_send, relay_recv,
):
    pos = place()
    x, y, zl, c, m = pos
    s = y * 4 + zl * 2 + c
    z = 2 * m + zl
    mine = y * 4 + x
    across = [(s, x, (m + k) % 4) for k in (2, 1, 3)]
    groups = [((s + i) % 16, (x + j) % 4, m) for i in range(16) for j in range(4) if i or j]
    owners = [
        ((x + i) % 4, (y + j) % 4, (m + k) % 4)
        for i in range(4) for j in range(4) for k in range(4) if i or j or k
    ]
    barrier = pltpu.get_barrier_semaphore()
    cross = [
        at((x + i) % 4, (y + j) % 4, zl, c, (m + k) % 4)
        for i in range(4) for j in range(4) for k in range(1, 4) if i or j
    ]
    column = [at(x, y, 1 - zl, c, (m + 1) % 4), at(x, y, 1 - zl, c, (m + 3) % 4)]
    peers = across + groups + cross + column
    for peer in peers:
        pl.semaphore_signal(barrier, inc=1, device_id=peer, device_id_type=MESH)

    own_text = pltpu.make_async_copy(text_hbm, text, local.at[0])
    own_text.start()

    gain1 = attn_gain[...].astype(F32)

    def norm_rows(i, carry):
        r = pl.ds(pl.multiple_of(i * 32, 32), 32)
        xn[r, :] = normed(patches[r, :].astype(F32), gain1).astype(BF)
        return carry

    lax.fori_loop(0, 16, norm_rows, 0)
    pl.semaphore_wait(barrier, len(peers))

    cp = Copies(send, recv)
    half_rows = pl.ds(pl.multiple_of((zl * 2 + c) * 80, 16), 80)
    hop0, finish0 = column_gather(
        cp, lambda k: (slice(None), slice(640 * k, 640 * (k + 1))), wout.at[half_rows], wout_all, pos
    )
    hop0(0)
    wout_all[z, c] = wout[half_rows, :]
    pieces, notes, biases = [], [], []
    for dy in range(4):
        for dx in range(4):
            if dx or dy:
                px, py = (x + dx) % 4, (y + dy) % 4
                cols = pl.ds(pl.multiple_of((py * 4 + px) * 128, 128), 128)
                pieces.append(cp.go(fc2.at[:, cols], f2p.at[mine], at(px, py, zl, c, m)))
    for peer in groups:
        spot = dall.at[pl.ds(pl.multiple_of((s * 4 + x) * 8, 8), 8)]
        notes.append(cp.go(dest, spot, peer))
    for dz in range(2):
        for dc in range(2):
            if dz or dc:
                biases.append(
                    cp.go(fc1_bias, ball.at[zl * 2 + c], at(x, y, (zl + dz) % 2, (c + dc) % 2, m))
                )
    f2p[mine] = fc2[:, pl.ds(pl.multiple_of(mine * 128, 128), 128)]
    dall[pl.ds(pl.multiple_of((s * 4 + x) * 8, 8), 8), :] = dest[...]
    ball[zl * 2 + c] = fc1_bias[...]

    lane = lax.broadcasted_iota(jnp.int32, (256, 320), 1)
    for t in range(2):
        xt = xn[256 * t : 256 * (t + 1), :]
        q, k, v = (dot(xt, wqkv[j], NT).astype(BF) for j in range(3))
        hop0(2 * t + 1)
        out = jnp.zeros((256, 320), F32)
        for h in range(4):
            inside = (lane >= 80 * h) & (lane < 80 * (h + 1))
            sc = dot(jnp.where(inside, q, jnp.zeros_like(q)), k, NT) * HEAD_DIM ** (-0.5)
            sc = sc + key_bias[t]
            sc = jnp.exp(sc - jnp.max(sc, axis=1, keepdims=True))
            w = (sc / jnp.sum(sc, axis=1, keepdims=True)).astype(BF)
            out = jnp.where(inside, dot(w, v), out)
            if h == 1:
                hop0(2 * t + 2)
        att[2 * t : 2 * t + 2] = out.astype(BF).reshape(2, 128, 320)
    parts = [cp.go(att.at[peer[2]], attr.at[m], peer) for peer in across]
    attr[m] = att[m]
    finish0()
    for copy in parts:
        copy.wait_recv()
    for k in range(4):
        w = wout_all[2 * k : 2 * k + 2].reshape(320, 1280)
        part = dot(attr[k], w)
        nrm[...] = part if k == 0 else nrm[...] + part
    gain2 = merge_gain[...].astype(F32)
    for i in range(4):
        r = pl.ds(pl.multiple_of(m * 128 + 32 * i, 32), 32)
        o = (patches[r, :].astype(F32) + nrm[32 * i : 32 * (i + 1), :]).astype(BF)
        o = normed(o.astype(F32), gain2)
        for b in range(10):
            turn[b, 32 * i : 32 * (i + 1), :] = o[:, 128 * b : 128 * (b + 1)]
    for p in range(4):
        for b in range(10):
            cols = slice(128 * b, 128 * (b + 1))
            blk1[p, :, cols] = turn[b, pl.ds(p, 32, stride=4), :].astype(BF)

    hop1, finish1 = column_gather(
        cp, lambda k: (slice(None), slice(640 * k, 640 * (k + 1))), fc1, fc1_all, pos
    )
    fc1_all[z, c] = fc1[...]
    plane_gather(cp, blk1, rows_all, hop1, pos)
    finish1()
    for copy in biases:
        copy.wait_recv()
    for p in range(4):
        part = dot(
            fc1_all[2 * p : 2 * p + 2].reshape(320, 1280), rows_all[p].reshape(512, 1280), NT
        )
        acc[0:320, :] = part if p == 0 else acc[0:320, :] + part
    for b in range(4):
        h = acc[80 * b : 80 * (b + 1), :] + ball[b][:, :1].astype(F32)
        blk2[b] = (0.5 * h * (1.0 + lax.erf(h * 0.5**0.5))).astype(BF)

    for copy in pieces:
        copy.wait_recv()
    hop2, finish2 = column_gather(
        cp, lambda k: (slice(8 * k, 8 * (k + 1)),), f2p, fc2_all, pos
    )
    fc2_all[z, c] = f2p[...]
    plane_gather(cp, blk2, hid_all, hop2, pos)
    finish2()

    onward = pltpu.make_async_remote_copy(
        src_ref=hidden_hbm, dst_ref=incoming, send_sem=relay_send, recv_sem=relay_recv,
        device_id=((s + 1) % 16, x, m), device_id_type=MESH,
    )

    @pl.when(s < 15)
    def _():
        onward.start()

    for b in range(4):
        zl_, c_ = b // 2, b % 2
        w = jnp.concatenate(
            [fc2_all[2 * k + zl_, c_].reshape(1280, 128) for k in range(4)], axis=1
        )
        part = dot(hid_all[b].reshape(1280, 512), w, TN)
        acc[...] = part if b == 0 else acc[...] + part
    for k in range(4):
        second[k] = acc[:, 128 * k : 128 * (k + 1)].astype(BF)

    cp3 = Copies(send3, recv3)

    def rows(px, py):
        return pl.ds(pl.multiple_of((py * 4 + px) * 32, 32), 32)

    home = (pl.ds(pl.multiple_of(m * 32, 32), 32), pl.ds(pl.multiple_of(mine * 128, 128), 128))
    moved = [
        cp3.go(second.at[pm, rows(px, py)], emb.at[home], at(px, py, zl, c, pm))
        for px, py, pm in owners
    ]
    emb[home] = second[m, rows(x, y)]
    for copy in moved:
        copy.wait_recv()
    bias2 = fc2_bias[...].astype(F32)
    for b in range(16):
        e = (emb[:, 128 * b : 128 * (b + 1)].astype(F32) + bias2[:, 128 * b : 128 * (b + 1)]).astype(BF)
        flat[pl.ds(b, 128, stride=16), :] = dot(pick[...], e)
    send_rows[...] = flat[...].astype(BF).reshape(64, 32, 128)
    moved = [
        cp3.go(send_rows.at[peer[0] * 4 + peer[1]], got.at[s * 4 + x], peer) for peer in groups
    ]
    got[s * 4 + x] = send_rows[s * 4 + x]
    for copy in notes:
        copy.wait_recv()
    d = dall[pl.ds(0, 64, stride=8), :]
    low = (s * 4 + x) * 512
    row = lax.broadcasted_iota(jnp.int32, (64, 512), 1)
    odd = lax.broadcasted_iota(jnp.int32, (64, 128), 1) % 2
    here = (d >= low) & (d < low + 512)
    puts = []
    for i in range(2):
        spot = jnp.max(jnp.where(here & (odd == i), (d - low).astype(F32), -1.0), axis=1, keepdims=True)
        puts.append((row == spot.astype(jnp.int32)).astype(F32).astype(BF))
    own_text.wait()

    @pl.when(s < 15)
    def _():
        onward.wait_send()

    @pl.when(s > 0)
    def _():
        onward.wait_recv()

    for copy in moved:
        copy.wait_recv()
    flat[...] = got[...].reshape(2048, 128).astype(F32)
    ones = jnp.ones((64, 128), BF)
    first = s == 0
    squares = [jnp.zeros((128, 128), F32) for _ in range(4)]
    hits = [
        dot(puts[0][:, 128 * r : 128 * (r + 1)], ones, TN)
        + dot(puts[1][:, 128 * r : 128 * (r + 1)], ones, TN)
        for r in range(4)
    ]
    for b in range(16):
        new = [flat[pl.ds(16 * i + b, 64, stride=32), :].astype(BF) for i in range(2)]
        cols = slice(128 * b, 128 * (b + 1))
        for r in range(4):
            rr = slice(128 * r, 128 * (r + 1))
            placed = dot(puts[0][:, rr], new[0], TN) + dot(puts[1][:, rr], new[1], TN)
            seq = jnp.where(hits[r] > 0.5, placed, text[rr, cols].astype(F32))
            seq_out[rr, cols] = seq.astype(BF)
            enter = jnp.where(first, seq, incoming[rr, cols].astype(F32))
            squares[r] = squares[r] + enter * enter
    sub = lax.broadcasted_iota(jnp.int32, (8, 128), 0)
    total = jnp.zeros((8, 128), F32)
    for r in range(4):
        line = jnp.broadcast_to(jnp.sum(squares[r], axis=1, keepdims=True), (128, 128)).T
        total = jnp.where(sub == r, line[0:8], total)
    sq_own[...] = total
    moved = [cp3.go(sq_own, sq_all.at[m], peer) for peer in across]
    sq_all[m] = total
    for copy in moved:
        copy.wait_recv()
    total = (sq_all[0] + sq_all[1]) + (sq_all[2] + sq_all[3])
    scale = lax.rsqrt(total / HID + llm_eps)
    gain3 = llm_gain[...].astype(F32)
    for r in range(4):
        by = jnp.broadcast_to(scale[r : r + 1, :], (128, 128)).T
        rr = slice(128 * r, 128 * (r + 1))
        for b in range(16):
            cols = slice(128 * b, 128 * (b + 1))
            enter = jnp.where(first, seq_out[rr, cols].astype(F32), incoming[rr, cols].astype(F32))
            layer_out[rr, cols] = (enter * by * gain3[:, cols]).astype(BF)
    cp.drain()
    cp3.drain()


def per_device(
    patches, patch_counts, dest_rows, qkv_weight, out_weight, attn_gain, merge_gain,
    fc1_weight, fc1_bias, fc2_weight, fc2_bias, text_embeds, section_hidden, llm_gain,
):
    merged, seq_rows = 128, text_embeds.shape[0]
    slot_in_tile = jnp.arange(merged, dtype=jnp.int32) % 64
    live = slot_in_tile * 4 < jnp.repeat(patch_counts, 64, total_repeat_length=merged)
    dest_live = jnp.broadcast_to(jnp.where(live, dest_rows, 2**30)[None, :], (8, merged))
    key_live = jnp.arange(256, dtype=jnp.int32)[None, None, :] < patch_counts[:, None, None]
    key_bias = jnp.where(key_live, 0.0, -1e30).astype(F32)
    slot = (dest_rows // seq_rows) * 2 + jnp.arange(merged, dtype=jnp.int32) % 2
    pick = (jnp.arange(merged, dtype=jnp.int32)[:, None] == slot[None, :]).astype(BF)
    vm = pl.BlockSpec(memory_space=pltpu.VMEM)
    hbm = pl.BlockSpec(memory_space=pl.ANY)
    dma = pltpu.SemaphoreType.DMA
    first_copies = 16 + 15 + 63 + 3 + 3 + 56 + 56
    return pl.pallas_call(
        step_kernel,
        out_shape=[jax.ShapeDtypeStruct((512, 2048), BF)] * 2,
        in_specs=[vm] * 13 + [hbm] * 2,
        out_specs=[vm] * 2,
        scratch_shapes=[
            pltpu.VMEM((512, 2048), BF),
            pltpu.VMEM((512, 2048), BF),
            pltpu.VMEM((512, 1280), BF),
            pltpu.VMEM((4, 128, 320), BF),
            pltpu.VMEM((4, 128, 320), BF),
            pltpu.VMEM((8, 2, 80, 1280), BF),
            pltpu.VMEM((16, 80, 128), BF),
            pltpu.VMEM((512, 128), jnp.int32),
            pltpu.VMEM((4, 80, 128), BF),
            pltpu.VMEM((128, 1280), F32),
            pltpu.VMEM((10, 128, 128), F32),
            pltpu.VMEM((4, 32, 1280), BF),
            pltpu.VMEM((4, 4, 4, 32, 1280), BF),
            pltpu.VMEM((8, 2, 80, 1280), BF),
            pltpu.VMEM((4, 80, 512), BF),
            pltpu.VMEM((4, 4, 4, 80, 512), BF),
            pltpu.VMEM((8, 2, 16, 80, 128), BF),
            pltpu.VMEM((512, 512), F32),
            pltpu.VMEM((4, 512, 128), BF),
            pltpu.VMEM((128, 2048), BF),
            pltpu.VMEM((2048, 128), F32),
            pltpu.VMEM((64, 32, 128), BF),
            pltpu.VMEM((64, 32, 128), BF),
            pltpu.VMEM((8, 128), F32),
            pltpu.VMEM((4, 8, 128), F32),
            dma((first_copies,)),
            dma((first_copies,)),
            dma((63 + 63 + 3,)),
            dma((63 + 63 + 3,)),
            dma((1,)),
            dma,
            dma,
        ],
        compiler_params=pltpu.CompilerParams(
            collective_id=1, has_side_effects=True, vmem_limit_bytes=60 * 2**20
        ),
    )(
        patches,
        key_bias,
        qkv_weight.transpose(1, 2, 0),
        out_weight,
        attn_gain[None, :],
        merge_gain[None, :],
        fc1_weight.T,
        jnp.broadcast_to(fc1_bias[:, None], (80, 128)),
        fc2_weight,
        fc2_bias[None, :],
        dest_live,
        pick,
        llm_gain[None, :],
        text_embeds,
        section_hidden,
    )


def solution(mesh):
    in_specs = (
        P(("section", "dp"), None),
        P(("section", "dp")),
        P(("section", "dp")),
        P(None, None, "mp"),
        P("mp", None),
        P(),
        P(),
        P("mp", ("section", "dp")),
        P(("section", "dp")),
        P(("section", "dp"), "mp"),
        P("mp"),
        P(("section", "dp"), "mp"),
        P(("section", "dp"), "mp"),
        P("mp"),
    )
    out_specs = (P(("section", "dp"), "mp"), P(("section", "dp"), "mp"))
    return jax.shard_map(
        per_device, mesh=mesh, in_specs=in_specs, out_specs=out_specs, check_vma=False
    )
```

```python
import jax
import jax.numpy as jnp
from jax import lax
from jax.experimental import pallas as pl
from jax.experimental.pallas import tpu as pltpu
from jax.sharding import PartitionSpec as P

HEAD_DIM = 80
HID = 8192
MESH = pl.DeviceIdType.MESH
BF = jnp.bfloat16
F32 = jnp.float32

vit_eps = 1e-06
llm_eps = 1e-06


def place():
    s = lax.axis_index("section")
    x = lax.axis_index("dp")
    m = lax.axis_index("mp")
    return x, s // 4, (s // 2) % 2, s % 2, m


def at(x, y, zl, c, m):
    return (y * 4 + zl * 2 + c, x, m)


def greet(peers):
    barrier = pltpu.get_barrier_semaphore()
    for peer in peers:
        pl.semaphore_signal(barrier, inc=1, device_id=peer, device_id_type=MESH)
    pl.semaphore_wait(barrier, len(peers))


class Copies:
    def __init__(self, send, recv):
        self.send, self.recv, self.all = send, recv, []

    def go(self, src, dst, peer):
        k = len(self.all)
        copy = pltpu.make_async_remote_copy(
            src_ref=src,
            dst_ref=dst,
            send_sem=self.send.at[k],
            recv_sem=self.recv.at[k],
            device_id=peer,
            device_id_type=MESH,
        )
        copy.start()
        self.all.append(copy)
        return copy

    def drain(self):
        for copy in self.all:
            copy.wait_send()


def column_gather(cp, halves, col, column, pos):
    x, y, zl, c, m = pos
    z = 2 * m + zl
    zs = [(z + k) % 8 for k in range(8)]

    def zdev(zz, cc):
        return at(x, y, zz % 2, cc, zz // 2)

    above, below, twin = zdev(zs[1], c), zdev(zs[7], c), zdev(z, 1 - c)
    up, down, side = {}, {}, []

    def hop(k):
        if k == 0:
            for j in range(2):
                src, dst = col.at[halves[j]], column.at[z, c].at[halves[j]]
                up[1, j] = cp.go(src, dst, above)
                down[1, j] = cp.go(src, dst, below)
            side.append(cp.go(col, column.at[z, c], twin))
            return
        for j in range(2):
            for ways, z_from, peer, last in ((up, zs[8 - k], above, 0), (down, zs[k % 8], below, 1)):
                if k < 4 or j == last:
                    ways[k, j].wait_recv()
                if k < 3 or (k == 3 and j == last):
                    ref = column.at[z_from, c].at[halves[j]]
                    ways[k + 1, j] = cp.go(ref, ref, peer)
        for z_from in [zs[8 - k], zs[k]][: 2 if k < 4 else 1]:
            ref = column.at[z_from, c]
            side.append(cp.go(ref, ref, twin))

    def finish():
        for copy in side:
            copy.wait_recv()

    return hop, finish


def plane_gather(cp, blk, plane, hop, drip, first, pos):
    x, y, zl, c, m = pos
    xs = [(x + k) % 4 for k in range(4)]
    ys = [(y + k) % 4 for k in range(4)]
    right, left = at(xs[1], y, zl, c, m), at(xs[3], y, zl, c, m)
    up, down = at(x, ys[1], zl, c, m), at(x, ys[3], zl, c, m)
    ahead = [[(right, left), (up, down)], [(up, down), (right, left)]]

    def block(v, a, b, lo, hi):
        fx, fy = (xs[a], ys[b]) if v == 0 else (xs[b], ys[a])
        return plane.at[2 * v + lo : 2 * v + hi, fy, fx]

    def push(v, axis, sgn, a, b, lo=0, hi=2, own=False):
        src = blk.at[2 * v + lo : 2 * v + hi] if own else block(v, a, b, lo, hi)
        return cp.go(src, block(v, a, b, lo, hi), ahead[v][axis][0 if sgn > 0 else 1])

    one, two, three, four = {}, {}, {}, {}
    for v in range(2):
        for g in (1, -1):
            one[v, g] = push(v, 0, g, 0, 0, own=True)
    for v in range(2):
        for g in (1, -1):
            three[v, 0, g] = push(v, 1, g, 0, 0, own=True)
    hop(0)
    plane[:, y, x] = blk[...]
    for g in (1, -1):
        for v in range(2):
            one[v, g].wait_recv()
            a = -g % 4
            two[v, g] = push(v, 0, g, a, 0, *((0, 1) if g > 0 else (1, 2)))
            for h in (1, -1):
                three[v, a, h] = push(v, 1, h, a, 0)
    hop(1)
    drip(first + 0)

    def opposite(a):
        for g in (1, -1):
            for v in range(2):
                three[v, a, g].wait_recv()
                four[v, a, g] = push(v, 1, g, a, -g % 4, *((0, 1) if g > 0 else (1, 2)))

    opposite(0)
    for v in range(2):
        for g in (1, -1):
            two[v, g].wait_recv()
        for h in (1, -1):
            three[v, 2, h] = push(v, 1, h, 2, 0)
    hop(2)
    drip(first + 1)
    opposite(3)
    opposite(1)
    hop(3)
    drip(first + 2)
    opposite(2)
    hop(4)
    drip(first + 3)
    for copy in four.values():
        copy.wait_recv()


BY_ROWS = (slice(0, 48), slice(48, 80))
NT = (((1,), (1,)), ((), ()))
TN = (((0,), (0,)), ((), ()))


def dot(a, b, dims=(((1,), (0,)), ((), ()))):
    return lax.dot_general(a, b, dims, preferred_element_type=F32)


def normed(v, gain):
    v = v - jnp.mean(v, axis=-1, keepdims=True)
    return v * lax.rsqrt(jnp.mean(v * v, axis=-1, keepdims=True) + vit_eps) * gain


def step_kernel(
    counts, patches, attn_gain, merge_gain, fc1_bias, fc2_bias, dest_rows, llm_gain,
    wqkv_hbm, wout_hbm, fc1_hbm, fc2_hbm, text_hbm, hidden_hbm,
    seq_hbm, layer_hbm,
    wqkv, wout, fc1, fc2, dest, bias1,
    text, incoming, stage, seq_out, layer_out,
    xn, att, attr, wout_all, f2p, dall, ball, nrm, turn, blk1, rows_all, fc1_all,
    blk2, hid_all, fc2_all, acc, second, emb, flat, send_rows, got, sq_own, sq_all,
    send, recv, send3, recv3, local, relay_send, relay_recv,
):
    pos = place()
    x, y, zl, c, m = pos
    s = y * 4 + zl * 2 + c
    z = 2 * m + zl
    mine = y * 4 + x
    across = [(s, x, (m + k) % 4) for k in (2, 1, 3)]
    groups = [((s + i) % 16, (x + j) % 4, m) for i in range(16) for j in range(4) if i or j]
    owners = [
        ((x + i) % 4, (y + j) % 4, (m + k) % 4)
        for i in range(4) for j in range(4) for k in range(4) if i or j or k
    ]
    barrier = pltpu.get_barrier_semaphore()
    cross = [
        at((x + i) % 4, (y + j) % 4, zl, c, (m + k) % 4)
        for i in range(4) for j in range(4) for k in range(1, 4) if i or j
    ]
    column = [at(x, y, 1 - zl, c, (m + 1) % 4), at(x, y, 1 - zl, c, (m + 3) % 4)]
    peers = across + groups + cross + column
    for peer in peers:
        pl.semaphore_signal(barrier, inc=1, device_id=peer, device_id_type=MESH)

    loads = [
        pltpu.make_async_copy(a, b, local.at[k])
        for k, (a, b) in enumerate(
            ((wout_hbm, wout), (fc2_hbm, fc2), (wqkv_hbm, wqkv), (fc1_hbm, fc1), (text_hbm, text))
        )
    ]
    for copy in loads:
        copy.start()

    j_lane = lax.broadcasted_iota(jnp.int32, (1, 128), 1)
    dest_row = dest_rows[...].reshape(1, 128)
    tile_count = jnp.where(j_lane < 64, counts[0], counts[1])
    live = (j_lane % 64) * 4 < tile_count
    dest[...] = jnp.broadcast_to(jnp.where(live, dest_row, 2**30), (8, 128))
    slot = (dest_row // 512) * 2 + j_lane % 2
    pick = (lax.broadcasted_iota(jnp.int32, (128, 128), 0) == slot).astype(F32).astype(BF)
    bias_row = fc1_bias[...].reshape(1, 80)
    top = lax.broadcasted_iota(jnp.int32, (8, 80), 0) == 0
    bias_row = jnp.where(top, bias_row.astype(F32), 0.0).astype(BF)
    bias1[...] = dot(bias_row, jnp.ones((8, 128), BF), TN).astype(BF)
    k_lane = lax.broadcasted_iota(jnp.int32, (1, 256), 1)
    key_bias = [jnp.where(k_lane < counts[t], 0.0, -1e30) for t in range(2)]

    gain1 = attn_gain[...].reshape(1, 1280).astype(F32)

    def norm_rows(i, carry):
        r = pl.ds(pl.multiple_of(i * 32, 32), 32)
        xn[r, :] = normed(patches[r, :].astype(F32), gain1).astype(BF)
        return carry

    lax.fori_loop(0, 16, norm_rows, 0)
    pl.semaphore_wait(barrier, len(peers))

    cp = Copies(send, recv)
    relay_to = [at(x, y, zl, 1, m), at(x, (y + 1) % 4, 1, 0, m), at(x, y, 1 - zl, 0, m)]
    relays = [
        pltpu.make_async_remote_copy(
            src_ref=hidden_hbm, dst_ref=ref, send_sem=relay_send.at[k], recv_sem=relay_recv.at[k],
            device_id=relay_to[k], device_id_type=MESH,
        )
        for k, ref in ((0, incoming), (1, stage))
    ]
    even_out, odd_out = (c == 1) & (zl == 0), (c == 0) & (zl == 1) & (y > 0)
    drips = []
    for k in range(16):
        r = slice(32 * k, 32 * (k + 1))
        drips.append(
            [
                pltpu.make_async_remote_copy(
                    src_ref=ref.at[r], dst_ref=incoming.at[r],
                    send_sem=relay_send.at[2 + k], recv_sem=relay_recv.at[2 + k],
                    device_id=relay_to[2], device_id_type=MESH,
                )
                for ref in (hidden_hbm, stage)
            ]
        )

    def drip(k):
        for j in (2 * k, 2 * k + 1):

            @pl.when(even_out)
            def _():
                drips[j][0].start()

            @pl.when(odd_out)
            def _():
                drips[j][1].start()

    loads[0].wait()
    half_rows = pl.ds(pl.multiple_of((zl * 2 + c) * 80, 16), 80)
    hop0, finish0 = column_gather(
        cp, BY_ROWS, wout.at[half_rows], wout_all, pos
    )
    hop0(0)

    @pl.when((c == 1) & (zl == 1) & (y < 3))
    def _():
        relays[1].start()

    @pl.when(c == 0)
    def _():
        relays[0].start()

    loads[1].wait()
    pieces, notes, biases = [], [], []
    for dy in range(4):
        for dx in range(4):
            if dx or dy:
                px, py = (x + dx) % 4, (y + dy) % 4
                cols = pl.ds(pl.multiple_of((py * 4 + px) * 128, 128), 128)
                pieces.append(cp.go(fc2.at[:, cols], f2p.at[mine], at(px, py, zl, c, m)))
    for peer in groups:
        spot = dall.at[pl.ds(pl.multiple_of((s * 4 + x) * 8, 8), 8)]
        notes.append(cp.go(dest, spot, peer))
    for dz in range(2):
        for dc in range(2):
            if dz or dc:
                biases.append(
                    cp.go(bias1, ball.at[zl * 2 + c], at(x, y, (zl + dz) % 2, (c + dc) % 2, m))
                )
    f2p[mine] = fc2[:, pl.ds(pl.multiple_of(mine * 128, 128), 128)]
    dall[pl.ds(pl.multiple_of((s * 4 + x) * 8, 8), 8), :] = dest[...]
    ball[zl * 2 + c] = bias1[...]
    wout_all[z, c] = wout[half_rows, :]
    loads[2].wait()

    lane = lax.broadcasted_iota(jnp.int32, (256, 320), 1)
    for t in range(2):
        xt = xn[256 * t : 256 * (t + 1), :]
        q, k, v = (dot(xt, wqkv[j], NT).astype(BF) for j in range(3))
        out = jnp.zeros((256, 320), F32)
        for h in range(4):
            inside = (lane >= 80 * h) & (lane < 80 * (h + 1))
            sc = dot(jnp.where(inside, q, jnp.zeros_like(q)), k, NT) * HEAD_DIM ** (-0.5)
            sc = sc + key_bias[t]
            sc = jnp.exp(sc - jnp.max(sc, axis=1, keepdims=True))
            w = (sc / jnp.sum(sc, axis=1, keepdims=True)).astype(BF)
            out = jnp.where(inside, dot(w, v), out)
            if t == 1 and h == 1:
                hop0(2)
        if t == 0:
            hop0(1)
        att[2 * t : 2 * t + 2] = out.astype(BF).reshape(2, 128, 320)
    parts = [cp.go(att.at[peer[2]], attr.at[m], peer) for peer in across]
    attr[m] = att[m]
    hop0(3)
    hop0(4)
    finish0()
    for copy in parts:
        copy.wait_recv()
    for k in range(4):
        w = wout_all[2 * k : 2 * k + 2].reshape(320, 1280)
        part = dot(attr[k], w)
        nrm[...] = part if k == 0 else nrm[...] + part
    gain2 = merge_gain[...].reshape(1, 1280).astype(F32)
    for i in range(4):
        r = pl.ds(pl.multiple_of(m * 128 + 32 * i, 32), 32)
        o = (patches[r, :].astype(F32) + nrm[32 * i : 32 * (i + 1), :]).astype(BF)
        o = normed(o.astype(F32), gain2)
        for b in range(10):
            turn[b, 32 * i : 32 * (i + 1), :] = o[:, 128 * b : 128 * (b + 1)]
    for p in range(4):
        for b in range(10):
            cols = slice(128 * b, 128 * (b + 1))
            blk1[p, :, cols] = turn[b, pl.ds(p, 32, stride=4), :].astype(BF)

    loads[3].wait()

    @pl.when(odd_out)
    def _():
        relays[1].wait_recv()

    hop1, finish1 = column_gather(cp, BY_ROWS, fc1, fc1_all, pos)
    fc1_all[z, c] = fc1[...]
    plane_gather(cp, blk1, rows_all, hop1, drip, 0, pos)
    finish1()
    for copy in biases:
        copy.wait_recv()
    for p in range(4):
        part = dot(
            fc1_all[2 * p : 2 * p + 2].reshape(320, 1280), rows_all[p].reshape(512, 1280), NT
        )
        acc[0:320, :] = part if p == 0 else acc[0:320, :] + part
    for b in range(4):
        h = acc[80 * b : 80 * (b + 1), :] + ball[b][:, :1].astype(F32)
        blk2[b] = (0.5 * h * (1.0 + lax.erf(h * 0.5**0.5))).astype(BF)

    for copy in pieces:
        copy.wait_recv()
    hop2, finish2 = column_gather(cp, (slice(0, 8), slice(8, 16)), f2p, fc2_all, pos)
    fc2_all[z, c] = f2p[...]
    plane_gather(cp, blk2, hid_all, hop2, drip, 4, pos)
    finish2()

    for b in range(4):
        zl_, c_ = b // 2, b % 2
        w = jnp.concatenate(
            [fc2_all[2 * k + zl_, c_].reshape(1280, 128) for k in range(4)], axis=1
        )
        part = dot(hid_all[b].reshape(1280, 512), w, TN)
        acc[...] = part if b == 0 else acc[...] + part
    for k in range(4):
        second[k] = acc[:, 128 * k : 128 * (k + 1)].astype(BF)

    cp3 = Copies(send3, recv3)

    def rows(px, py):
        return pl.ds(pl.multiple_of((py * 4 + px) * 32, 32), 32)

    home = (pl.ds(pl.multiple_of(m * 32, 32), 32), pl.ds(pl.multiple_of(mine * 128, 128), 128))
    moved = [
        cp3.go(second.at[pm, rows(px, py)], emb.at[home], at(px, py, zl, c, pm))
        for px, py, pm in owners
    ]
    emb[home] = second[m, rows(x, y)]
    for copy in moved:
        copy.wait_recv()
    bias2 = fc2_bias[...].reshape(1, 2048).astype(F32)
    for b in range(16):
        e = (emb[:, 128 * b : 128 * (b + 1)].astype(F32) + bias2[:, 128 * b : 128 * (b + 1)]).astype(BF)
        flat[pl.ds(b, 128, stride=16), :] = dot(pick, e)
    send_rows[...] = flat[...].astype(BF).reshape(64, 32, 128)
    moved = [
        cp3.go(send_rows.at[peer[0] * 4 + peer[1]], got.at[s * 4 + x], peer) for peer in groups
    ]
    got[s * 4 + x] = send_rows[s * 4 + x]
    for copy in notes:
        copy.wait_recv()
    d = dall[pl.ds(0, 64, stride=8), :]
    low = (s * 4 + x) * 512
    row = lax.broadcasted_iota(jnp.int32, (64, 512), 1)
    odd = lax.broadcasted_iota(jnp.int32, (64, 128), 1) % 2
    here = (d >= low) & (d < low + 512)
    puts = []
    for i in range(2):
        spot = jnp.max(jnp.where(here & (odd == i), (d - low).astype(F32), -1.0), axis=1, keepdims=True)
        puts.append((row == spot.astype(jnp.int32)).astype(F32).astype(BF))
    loads[4].wait()

    @pl.when(c == 1)
    def _():
        relays[0].wait_recv()

    @pl.when((c == 0) & (s > 0))
    def _():
        for k in range(16):
            drips[k][0].wait_recv()

    for copy in moved:
        copy.wait_recv()
    flat[...] = got[...].reshape(2048, 128).astype(F32)
    ones = jnp.ones((64, 128), BF)
    first = s == 0
    squares = [jnp.zeros((128, 128), F32) for _ in range(4)]
    hits = [
        dot(puts[0][:, 128 * r : 128 * (r + 1)], ones, TN)
        + dot(puts[1][:, 128 * r : 128 * (r + 1)], ones, TN)
        for r in range(4)
    ]
    for b in range(16):
        new = [flat[pl.ds(16 * i + b, 64, stride=32), :].astype(BF) for i in range(2)]
        cols = slice(128 * b, 128 * (b + 1))
        for r in range(4):
            rr = slice(128 * r, 128 * (r + 1))
            placed = dot(puts[0][:, rr], new[0], TN) + dot(puts[1][:, rr], new[1], TN)
            seq = jnp.where(hits[r] > 0.5, placed, text[rr, cols].astype(F32))
            seq_out[rr, cols] = seq.astype(BF)
            enter = jnp.where(first, seq, incoming[rr, cols].astype(F32))
            squares[r] = squares[r] + enter * enter
    seq_save = pltpu.make_async_copy(seq_out, seq_hbm, local.at[0])
    seq_save.start()
    sub = lax.broadcasted_iota(jnp.int32, (8, 128), 0)
    total = jnp.zeros((8, 128), F32)
    for r in range(4):
        line = jnp.broadcast_to(jnp.sum(squares[r], axis=1, keepdims=True), (128, 128)).T
        total = jnp.where(sub == r, line[0:8], total)
    sq_own[...] = total
    moved = [cp3.go(sq_own, sq_all.at[m], peer) for peer in across]
    sq_all[m] = total
    for copy in moved:
        copy.wait_recv()
    total = (sq_all[0] + sq_all[1]) + (sq_all[2] + sq_all[3])
    scale = lax.rsqrt(total / HID + llm_eps)
    gain3 = llm_gain[...].reshape(1, 2048).astype(F32)
    saves = []
    for r in range(4):
        by = jnp.broadcast_to(scale[r : r + 1, :], (128, 128)).T
        rr = slice(128 * r, 128 * (r + 1))
        for b in range(16):
            cols = slice(128 * b, 128 * (b + 1))
            enter = jnp.where(first, seq_out[rr, cols].astype(F32), incoming[rr, cols].astype(F32))
            layer_out[rr, cols] = (enter * by * gain3[:, cols]).astype(BF)
        saves.append(pltpu.make_async_copy(layer_out.at[rr], layer_hbm.at[rr], local.at[1 + r]))
        saves[-1].start()
    cp.drain()
    cp3.drain()

    @pl.when(c == 0)
    def _():
        relays[0].wait_send()

    @pl.when((c == 1) & (zl == 1) & (y < 3))
    def _():
        relays[1].wait_send()

    @pl.when(even_out | odd_out)
    def _():
        for k in range(16):
            drips[k][0].wait_send()

    seq_save.wait()
    for copy in saves:
        copy.wait()


def per_device(
    patches, patch_counts, dest_rows, qkv_weight, out_weight, attn_gain, merge_gain,
    fc1_weight, fc1_bias, fc2_weight, fc2_bias, text_embeds, section_hidden, llm_gain,
):
    vm = pl.BlockSpec(memory_space=pltpu.VMEM)
    hbm = pl.BlockSpec(memory_space=pl.ANY)
    dma = pltpu.SemaphoreType.DMA
    first_copies = 23 + 15 + 63 + 3 + 3 + 63 + 63
    return pl.pallas_call(
        step_kernel,
        out_shape=[jax.ShapeDtypeStruct((512, 2048), BF)] * 2,
        in_specs=[pl.BlockSpec(memory_space=pltpu.SMEM)] + [vm] * 7 + [hbm] * 6,
        out_specs=[hbm] * 2,
        scratch_shapes=[
            pltpu.VMEM((3, 320, 1280), BF),
            pltpu.VMEM((320, 1280), BF),
            pltpu.VMEM((80, 1280), BF),
            pltpu.VMEM((80, 2048), BF),
            pltpu.VMEM((8, 128), jnp.int32),
            pltpu.VMEM((80, 128), BF),
            pltpu.VMEM((512, 2048), BF),
            pltpu.VMEM((512, 2048), BF),
            pltpu.VMEM((512, 2048), BF),
            pltpu.VMEM((512, 2048), BF),
            pltpu.VMEM((512, 2048), BF),
            pltpu.VMEM((512, 1280), BF),
            pltpu.VMEM((4, 128, 320), BF),
            pltpu.VMEM((4, 128, 320), BF),
            pltpu.VMEM((8, 2, 80, 1280), BF),
            pltpu.VMEM((16, 80, 128), BF),
            pltpu.VMEM((512, 128), jnp.int32),
            pltpu.VMEM((4, 80, 128), BF),
            pltpu.VMEM((128, 1280), F32),
            pltpu.VMEM((10, 128, 128), F32),
            pltpu.VMEM((4, 32, 1280), BF),
            pltpu.VMEM((4, 4, 4, 32, 1280), BF),
            pltpu.VMEM((8, 2, 80, 1280), BF),
            pltpu.VMEM((4, 80, 512), BF),
            pltpu.VMEM((4, 4, 4, 80, 512), BF),
            pltpu.VMEM((8, 2, 16, 80, 128), BF),
            pltpu.VMEM((512, 512), F32),
            pltpu.VMEM((4, 512, 128), BF),
            pltpu.VMEM((128, 2048), BF),
            pltpu.VMEM((2048, 128), F32),
            pltpu.VMEM((64, 32, 128), BF),
            pltpu.VMEM((64, 32, 128), BF),
            pltpu.VMEM((8, 128), F32),
            pltpu.VMEM((4, 8, 128), F32),
            dma((first_copies,)),
            dma((first_copies,)),
            dma((63 + 63 + 3,)),
            dma((63 + 63 + 3,)),
            dma((5,)),
            dma((18,)),
            dma((18,)),
        ],
        compiler_params=pltpu.CompilerParams(
            collective_id=1, has_side_effects=True, vmem_limit_bytes=60 * 2**20
        ),
    )(
        patch_counts, patches, attn_gain, merge_gain, fc1_bias, fc2_bias, dest_rows, llm_gain,
        qkv_weight.transpose(1, 2, 0), out_weight, fc1_weight.T, fc2_weight,
        text_embeds, section_hidden,
    )


def solution(mesh):
    in_specs = (
        P(("section", "dp"), None),
        P(("section", "dp")),
        P(("section", "dp")),
        P(None, None, "mp"),
        P("mp", None),
        P(),
        P(),
        P("mp", ("section", "dp")),
        P(("section", "dp")),
        P(("section", "dp"), "mp"),
        P("mp"),
        P(("section", "dp"), "mp"),
        P(("section", "dp"), "mp"),
        P("mp"),
    )
    out_specs = (P(("section", "dp"), "mp"), P(("section", "dp"), "mp"))
    return jax.shard_map(
        per_device, mesh=mesh, in_specs=in_specs, out_specs=out_specs, check_vma=False
    )
```

```python
import jax
import jax.numpy as jnp
from jax import lax
from jax.experimental import pallas as pl
from jax.experimental.pallas import tpu as pltpu
from jax.sharding import PartitionSpec as P

HEAD_DIM = 80
HID = 8192
MESH = pl.DeviceIdType.MESH
BF = jnp.bfloat16
F32 = jnp.float32

vit_eps = 1e-06
llm_eps = 1e-06


def place():
    s = lax.axis_index("section")
    x = lax.axis_index("dp")
    m = lax.axis_index("mp")
    return x, s // 4, (s // 2) % 2, s % 2, m


def at(x, y, zl, c, m):
    return (y * 4 + zl * 2 + c, x, m)


class Wire:
    def __init__(self, send, recv):
        self.send, self.recv, self.sends, self.recvs = send, recv, 0, 0

    def batch(self, sent, shared=None):
        k = self.sends
        self.sends += 1
        if shared is not None:
            shared, self.recvs = self.recvs, self.recvs + 1
        return Batch(self, k, sent, shared)


class Batch:
    def __init__(self, wire, k, sent, shared):
        self.wire, self.sem, self.sent, self.shared = wire, wire.send.at[k], sent, shared

    def describe(self, src, dst, k, peer):
        return pltpu.make_async_remote_copy(
            src_ref=src, dst_ref=dst, send_sem=self.sem, recv_sem=self.wire.recv.at[k],
            device_id=peer, device_id_type=MESH,
        )

    def go(self, src, dst, peer):
        k = self.shared
        if k is None:
            k, self.wire.recvs = self.wire.recvs, self.wire.recvs + 1
        copy = self.describe(src, dst, k, peer)
        copy.start()
        self.peer = peer
        return copy

    def wait_recv(self):
        self.describe(self.sent, self.sent, self.shared, self.peer).wait_recv()

    def wait_send(self):
        self.describe(self.sent, self.sent, 0, self.peer).wait_send()


def column_gather(wire, ring_bytes, side_bytes, halves, col, column, pos, upward=(0,)):
    x, y, zl, c, m = pos
    z = 2 * m + zl
    zs = [(z + k) % 8 for k in range(8)]

    def zdev(zz, cc):
        return at(x, y, zz % 2, cc, zz // 2)

    above, below, twin = zdev(zs[1], c), zdev(zs[7], c), zdev(z, 1 - c)
    up, down = {}, {}
    up_far, down_far = upward, tuple(j for j in range(2) if j not in upward)
    ring, side = wire.batch(ring_bytes), wire.batch(side_bytes, shared=True)

    def hop(k):
        if k == 0:
            for j in range(2):
                src, dst = col.at[halves[j]], column.at[z, c].at[halves[j]]
                up[1, j] = ring.go(src, dst, above)
                down[1, j] = ring.go(src, dst, below)
            side.go(col, column.at[z, c], twin)
            return
        for j in range(2):
            for ways, z_from, peer, far in ((up, zs[8 - k], above, up_far), (down, zs[k], below, down_far)):
                if k < 4 or j in far:
                    ways[k, j].wait_recv()
                if k < 3 or (k == 3 and j in far):
                    ref = column.at[z_from, c].at[halves[j]]
                    ways[k + 1, j] = ring.go(ref, ref, peer)
        for z_from in [zs[8 - k], zs[k]][: 2 if k < 4 else 1]:
            ref = column.at[z_from, c]
            side.go(ref, ref, twin)

    return hop, side.wait_recv, [ring, side]


def shared_gather(wire, col, column, half_bytes, side_bytes, pos):
    x, y, zl, c, m = pos
    z = 2 * m + zl
    zs = [(z + k) % 8 for k in range(8)]

    def zdev(zz, cc):
        return at(x, y, zz % 2, cc, zz // 2)

    above, below, twin = zdev(zs[1], c), zdev(zs[7], c), zdev(z, 1 - c)
    right, left = at((x + 1) % 4, y, zl, c, m), at((x + 3) % 4, y, zl, c, m)
    mine = pl.ds(pl.multiple_of((x % 2) * 640, 128), 640)
    other = pl.ds(pl.multiple_of((1 - x % 2) * 640, 128), 640)
    ring, across = wire.batch(half_bytes), wire.batch(half_bytes)
    side = wire.batch(side_bytes, shared=True)
    ways = {}
    crossed = []

    def hop(k):
        if k == 0:
            dst = column.at[z, c].at[:, mine]
            ways["up", 1] = ring.go(col.at[:, mine], dst, above)
            ways["down", 1] = ring.go(col.at[:, mine], dst, below)
            side.go(col, column.at[z, c], twin)
            return
        for way, z_from, peer, beside, end in (
            ("up", zs[8 - k], above, right, 4), ("down", zs[k], below, left, 3)
        ):
            if k <= end:
                ways[way, k].wait_recv()
                ref = column.at[z_from, c].at[:, mine]
                if k < end:
                    ways[way, k + 1] = ring.go(ref, ref, peer)
                crossed.append((across.go(ref, ref, beside), column.at[z_from, c].at[:, other]))
                side.go(ref, ref, twin)

    def finish():
        for copy, ref in crossed:
            copy.wait_recv()
            side.go(ref, ref, twin)
        side.wait_recv()

    return hop, finish, [ring, across, side]


def plane_gather(cp, blk, plane, points, pos):
    x, y, zl, c, m = pos
    xs = [(x + k) % 4 for k in range(4)]
    ys = [(y + k) % 4 for k in range(4)]
    right, left = at(xs[1], y, zl, c, m), at(xs[3], y, zl, c, m)
    up, down = at(x, ys[1], zl, c, m), at(x, ys[3], zl, c, m)
    ahead = [[(right, left), (up, down)], [(up, down), (right, left)]]

    def block(v, a, b, lo, hi):
        fx, fy = (xs[a], ys[b]) if v == 0 else (xs[b], ys[a])
        return plane.at[2 * v + lo : 2 * v + hi, fy, fx]

    def push(v, axis, sgn, a, b, lo=0, hi=2, own=False):
        src = blk.at[2 * v + lo : 2 * v + hi] if own else block(v, a, b, lo, hi)
        return cp.go(src, block(v, a, b, lo, hi), ahead[v][axis][0 if sgn > 0 else 1])

    one, two, three, four = {}, {}, {}, {}
    for v in range(2):
        for g in (1, -1):
            one[v, g] = push(v, 0, g, 0, 0, own=True)
    for v in range(2):
        for g in (1, -1):
            three[v, 0, g] = push(v, 1, g, 0, 0, own=True)
    points[0]()
    plane[:, y, x] = blk[...]
    for g in (1, -1):
        for v in range(2):
            one[v, g].wait_recv()
            a = -g % 4
            two[v, g] = push(v, 0, g, a, 0, *((0, 1) if g > 0 else (1, 2)))
            for h in (1, -1):
                three[v, a, h] = push(v, 1, h, a, 0)
    points[1]()

    def opposite(a):
        for g in (1, -1):
            for v in range(2):
                three[v, a, g].wait_recv()
                four[v, a, g] = push(v, 1, g, a, -g % 4, *((0, 1) if g > 0 else (1, 2)))

    opposite(0)
    for v in range(2):
        for g in (1, -1):
            two[v, g].wait_recv()
        for h in (1, -1):
            three[v, 2, h] = push(v, 1, h, 2, 0)
    points[2]()
    opposite(3)
    opposite(1)
    points[3]()
    opposite(2)
    points[4]()
    for copy in four.values():
        copy.wait_recv()


BY_ROWS = (slice(0, 48), slice(48, 80))
NT = (((1,), (1,)), ((), ()))
TN = (((0,), (0,)), ((), ()))


def dot(a, b, dims=(((1,), (0,)), ((), ()))):
    return lax.dot_general(a, b, dims, preferred_element_type=F32)


def normed(v, gain):
    v = v - jnp.mean(v, axis=-1, keepdims=True)
    return v * lax.rsqrt(jnp.mean(v * v, axis=-1, keepdims=True) + vit_eps) * gain


def step_kernel(
    counts, patches, attn_gain, merge_gain, fc1_bias, fc2_bias, dest_rows, llm_gain,
    wqkv_hbm, wout_hbm, fc1_hbm, fc2_hbm, text_hbm, hidden_hbm,
    seq_out, layer_out,
    wqkv, wout, fc1, fc2, dest, bias1,
    text, incoming, stage,
    xn, att, attr, wout_all, f2p, dall, ball, nrm, turn, blk1, rows_all, fc1_all,
    blk2, hid_all, fc2_all, acc, second, emb, flat, send_rows, got, sq_own, sq_all,
    send, recv, local, relay_send, relay_recv,
):
    pos = place()
    x, y, zl, c, m = pos
    s = y * 4 + zl * 2 + c
    z = 2 * m + zl
    mine = y * 4 + x
    across = [(s, x, (m + k) % 4) for k in (2, 1, 3)]
    groups = [((s + i) % 16, (x + j) % 4, m) for i in range(16) for j in range(4) if i or j]
    owners = [
        ((x + i) % 4, (y + j) % 4, (m + k) % 4)
        for i in range(4) for j in range(4) for k in range(4) if i or j or k
    ]
    barrier = pltpu.get_barrier_semaphore()
    cross = [
        at((x + i) % 4, (y + j) % 4, zl, c, (m + k) % 4)
        for i in range(4) for j in range(4) for k in range(1, 4) if i or j
    ]
    column = [at(x, y, 1 - zl, c, (m + 1) % 4), at(x, y, 1 - zl, c, (m + 3) % 4)]
    peers = across + groups + cross + column
    for peer in peers:
        pl.semaphore_signal(barrier, inc=1, device_id=peer, device_id_type=MESH)

    loads = [
        pltpu.make_async_copy(a, b, local.at[k])
        for k, (a, b) in enumerate(
            ((wout_hbm, wout), (fc2_hbm, fc2), (wqkv_hbm, wqkv), (fc1_hbm, fc1), (text_hbm, text))
        )
    ]
    for copy in loads:
        copy.start()

    pl.semaphore_wait(barrier, len(peers))

    wire = Wire(send, recv)
    relay_to = [at(x, y, zl, 1, m), at(x, (y + 1) % 4, 1, 0, m), at(x, y, 1 - zl, 0, m)]
    relays = [
        pltpu.make_async_remote_copy(
            src_ref=hidden_hbm, dst_ref=ref, send_sem=relay_send.at[k], recv_sem=relay_recv.at[k],
            device_id=relay_to[k], device_id_type=MESH,
        )
        for k, ref in ((0, incoming), (1, stage))
    ]
    even_out, odd_out = (c == 1) & (zl == 0), (c == 0) & (zl == 1) & (y > 0)
    drips = []
    for k in range(16):
        r = slice(32 * k, 32 * (k + 1))
        drips.append(
            [
                pltpu.make_async_remote_copy(
                    src_ref=ref.at[r], dst_ref=incoming.at[r],
                    send_sem=relay_send.at[2], recv_sem=relay_recv.at[2],
                    device_id=relay_to[2], device_id_type=MESH,
                )
                for ref in (hidden_hbm, stage)
            ]
        )
    all_drips = pltpu.make_async_remote_copy(
        src_ref=stage, dst_ref=incoming, send_sem=relay_send.at[2], recv_sem=relay_recv.at[2],
        device_id=relay_to[2], device_id_type=MESH,
    )

    def drip(k):
        for j in range((0, 2, 4, 6, 7, 9, 11, 12, 12)[k], (2, 4, 6, 7, 9, 11, 12, 12, 16)[k]):

            @pl.when(even_out)
            def _():
                drips[j][0].start()

            @pl.when(odd_out)
            def _():
                drips[j][1].start()

    loads[0].wait()
    half_rows = pl.ds(pl.multiple_of((zl * 2 + c) * 80, 16), 80)
    hop0, finish0, batches = shared_gather(
        wire, wout.at[half_rows], wout_all, fc1_all.at[0:7, 0, :, 0:640], fc1_all.at[0:4], pos
    )
    hop0(0)

    @pl.when((c == 1) & (zl == 1) & (y < 3))
    def _():
        relays[1].start()

    @pl.when(c == 0)
    def _():
        relays[0].start()

    loads[1].wait()
    pieces = wire.batch(f2p.at[0:15], shared=True)
    notes = wire.batch(dall.at[0:63], shared=True)
    biases = wire.batch(ball.at[0:3], shared=True)
    parts = wire.batch(attr.at[0:3], shared=True)
    batches += [pieces, notes, biases, parts]
    for dy in range(4):
        for dx in range(4):
            if dx or dy:
                px, py = (x + dx) % 4, (y + dy) % 4
                cols = pl.ds(pl.multiple_of((py * 4 + px) * 128, 128), 128)
                pieces.go(fc2.at[:, cols], f2p.at[mine], at(px, py, zl, c, m))
    j_lane = lax.broadcasted_iota(jnp.int32, (1, 128), 1)
    dest_row = dest_rows[...].reshape(1, 128)
    tile_count = jnp.where(j_lane < 64, counts[0], counts[1])
    live = (j_lane % 64) * 4 < tile_count
    dest[...] = jnp.where(live, dest_row, 2**30)
    slot = (dest_row // 512) * 2 + j_lane % 2
    pick = (lax.broadcasted_iota(jnp.int32, (128, 128), 0) == slot).astype(F32).astype(BF)
    bias_row = fc1_bias[...].reshape(1, 80)
    top = lax.broadcasted_iota(jnp.int32, (8, 80), 0) == 0
    bias_row = jnp.where(top, bias_row.astype(F32), 0.0).astype(BF)
    bias1[...] = dot(bias_row, jnp.ones((8, 128), BF), TN).astype(BF)
    k_lane = lax.broadcasted_iota(jnp.int32, (1, 256), 1)
    key_bias = [jnp.where(k_lane < counts[t], 0.0, -1e30) for t in range(2)]

    for peer in groups:
        notes.go(dest, dall.at[s * 4 + x], peer)
    for dz in range(2):
        for dc in range(2):
            if dz or dc:
                biases.go(bias1, ball.at[zl * 2 + c], at(x, y, (zl + dz) % 2, (c + dc) % 2, m))
    f2p[mine] = fc2[:, pl.ds(pl.multiple_of(mine * 128, 128), 128)]
    dall[s * 4 + x] = dest[...]
    ball[zl * 2 + c] = bias1[...]
    wout_all[z, c] = wout[half_rows, :]
    loads[2].wait()

    gain1 = attn_gain[...].reshape(1, 1280).astype(F32)

    def norm_rows(i, carry):
        r = pl.ds(pl.multiple_of(i * 32, 32), 32)
        xn[r, :] = normed(patches[r, :].astype(F32), gain1).astype(BF)
        return carry

    lax.fori_loop(0, 16, norm_rows, 0)

    hop0(1)
    lane = lax.broadcasted_iota(jnp.int32, (256, 320), 1)
    for t in range(2):
        xt = xn[256 * t : 256 * (t + 1), :]
        q, k, v = (dot(xt, wqkv[j], NT).astype(BF) for j in range(3))
        out = jnp.zeros((256, 320), F32)
        for h in range(4):
            inside = (lane >= 80 * h) & (lane < 80 * (h + 1))
            sc = dot(jnp.where(inside, q, jnp.zeros_like(q)), k, NT) * HEAD_DIM ** (-0.5)
            sc = sc + key_bias[t]
            sc = jnp.exp(sc - jnp.max(sc, axis=1, keepdims=True))
            w = (sc / jnp.sum(sc, axis=1, keepdims=True)).astype(BF)
            out = jnp.where(inside, dot(w, v), out)
        att[2 * t : 2 * t + 2] = out.astype(BF).reshape(2, 128, 320)
    for peer in across:
        parts.go(att.at[peer[2]], attr.at[m], peer)
    attr[m] = att[m]
    for k in range(2, 5):
        hop0(k)
    finish0()
    parts.wait_recv()
    for k in range(4):
        w = wout_all[2 * k : 2 * k + 2].reshape(320, 1280)
        part = dot(attr[k], w)
        nrm[...] = part if k == 0 else nrm[...] + part
    gain2 = merge_gain[...].reshape(1, 1280).astype(F32)
    for i in range(4):
        r = pl.ds(pl.multiple_of(m * 128 + 32 * i, 32), 32)
        o = (patches[r, :].astype(F32) + nrm[32 * i : 32 * (i + 1), :]).astype(BF)
        o = normed(o.astype(F32), gain2)
        for b in range(10):
            turn[b, 32 * i : 32 * (i + 1), :] = o[:, 128 * b : 128 * (b + 1)]
    for p in range(4):
        for b in range(10):
            cols = slice(128 * b, 128 * (b + 1))
            blk1[p, :, cols] = turn[b, pl.ds(p, 32, stride=4), :].astype(BF)

    loads[3].wait()

    @pl.when(odd_out)
    def _():
        relays[1].wait_recv()

    hop1, finish1, more = column_gather(
        wire, fc1_all.at[0:7, 0], fc1_all.at[0:4], BY_ROWS, fc1, fc1_all, pos
    )
    planes = [wire.batch(fc2_all.at[:, :, 0:15]) for _ in range(2)]
    batches += more + planes
    fc1_all[z, c] = fc1[...]

    def point(*calls):
        def run():
            for call, k in calls:
                call(k)

        return run

    pieces.wait_recv()
    hop2, finish2, more = column_gather(
        wire, fc2_all.at[0:7, 0], fc2_all.at[0:4], (slice(0, 8), slice(8, 16)), f2p, fc2_all, pos
    )
    batches += more
    fc2_all[z, c] = f2p[...]
    plane_gather(
        planes[0],
        blk1,
        rows_all,
        [
            point((hop1, 0)),
            point((hop1, 1), (drip, 0)),
            point((hop1, 2), (drip, 1)),
            point((hop1, 3), (drip, 2)),
            point((hop1, 4), (hop2, 0), (drip, 3)),
        ],
        pos,
    )
    finish1()
    biases.wait_recv()
    for p in range(4):
        part = dot(
            fc1_all[2 * p : 2 * p + 2].reshape(320, 1280), rows_all[p].reshape(512, 1280), NT
        )
        acc[0:320, :] = part if p == 0 else acc[0:320, :] + part
    for b in range(4):
        h = acc[80 * b : 80 * (b + 1), :] + ball[b][:, :1].astype(F32)
        blk2[b] = (0.5 * h * (1.0 + lax.erf(h * 0.5**0.5))).astype(BF)

    plane_gather(
        planes[1],
        blk2,
        hid_all,
        [
            point(),
            point((hop2, 1), (drip, 4)),
            point((hop2, 2), (drip, 5)),
            point((hop2, 3), (drip, 6)),
            point((hop2, 4), (drip, 7)),
        ],
        pos,
    )
    finish2()

    for b in range(4):
        zl_, c_ = b // 2, b % 2
        w = jnp.concatenate(
            [fc2_all[2 * k + zl_, c_].reshape(1280, 128) for k in range(4)], axis=1
        )
        part = dot(hid_all[b].reshape(1280, 512), w, TN)
        acc[...] = part if b == 0 else acc[...] + part
    for k in range(4):
        second[k] = acc[:, 128 * k : 128 * (k + 1)].astype(BF)

    homes = wire.batch(got.at[0:63], shared=True)
    picked = wire.batch(got.at[0:63], shared=True)
    sums = wire.batch(sq_all.at[0:3], shared=True)
    batches += [homes, picked, sums]

    def rows(px, py):
        return pl.ds(pl.multiple_of((py * 4 + px) * 32, 32), 32)

    home = (pl.ds(pl.multiple_of(m * 32, 32), 32), pl.ds(pl.multiple_of(mine * 128, 128), 128))
    for px, py, pm in owners:
        homes.go(second.at[pm, rows(px, py)], emb.at[home], at(px, py, zl, c, pm))
    emb[home] = second[m, rows(x, y)]
    homes.wait_recv()
    bias2 = fc2_bias[...].reshape(1, 2048).astype(F32)
    for b in range(16):
        e = (emb[:, 128 * b : 128 * (b + 1)].astype(F32) + bias2[:, 128 * b : 128 * (b + 1)]).astype(BF)
        flat[pl.ds(b, 128, stride=16), :] = dot(pick, e)
    send_rows[...] = flat[...].astype(BF).reshape(64, 32, 128)
    for peer in groups:
        picked.go(send_rows.at[peer[0] * 4 + peer[1]], got.at[s * 4 + x], peer)
    drip(8)
    got[s * 4 + x] = send_rows[s * 4 + x]
    notes.wait_recv()
    d = dall[...].reshape(64, 128)
    low = (s * 4 + x) * 512
    row = lax.broadcasted_iota(jnp.int32, (64, 512), 1)
    odd = lax.broadcasted_iota(jnp.int32, (64, 128), 1) % 2
    here = (d >= low) & (d < low + 512)
    puts = []
    for i in range(2):
        spot = jnp.max(jnp.where(here & (odd == i), (d - low).astype(F32), -1.0), axis=1, keepdims=True)
        puts.append((row == spot.astype(jnp.int32)).astype(F32).astype(BF))
    loads[4].wait()

    @pl.when(c == 1)
    def _():
        relays[0].wait_recv()

    @pl.when((c == 0) & (s > 0))
    def _():
        all_drips.wait_recv()

    picked.wait_recv()
    flat[...] = got[...].reshape(2048, 128).astype(F32)
    ones = jnp.ones((64, 128), BF)
    first = s == 0
    squares = [jnp.zeros((128, 128), F32) for _ in range(4)]
    hits = [
        dot(puts[0][:, 128 * r : 128 * (r + 1)], ones, TN)
        + dot(puts[1][:, 128 * r : 128 * (r + 1)], ones, TN)
        for r in range(4)
    ]
    for b in range(16):
        new = [flat[pl.ds(16 * i + b, 64, stride=32), :].astype(BF) for i in range(2)]
        cols = slice(128 * b, 128 * (b + 1))
        for r in range(4):
            rr = slice(128 * r, 128 * (r + 1))
            placed = dot(puts[0][:, rr], new[0], TN) + dot(puts[1][:, rr], new[1], TN)
            seq = jnp.where(hits[r] > 0.5, placed, text[rr, cols].astype(F32))
            seq_out[rr, cols] = seq.astype(BF)
            enter = jnp.where(first, seq, incoming[rr, cols].astype(F32))
            squares[r] = squares[r] + enter * enter
    sub = lax.broadcasted_iota(jnp.int32, (8, 128), 0)
    total = jnp.zeros((8, 128), F32)
    for r in range(4):
        line = jnp.broadcast_to(jnp.sum(squares[r], axis=1, keepdims=True), (128, 128)).T
        total = jnp.where(sub == r, line[0:8], total)
    sq_own[...] = total
    for peer in across:
        sums.go(sq_own, sq_all.at[m], peer)
    sq_all[m] = total
    sums.wait_recv()
    total = (sq_all[0] + sq_all[1]) + (sq_all[2] + sq_all[3])
    scale = lax.rsqrt(total / HID + llm_eps)
    gain3 = llm_gain[...].reshape(1, 2048).astype(F32)
    for r in range(4):
        by = jnp.broadcast_to(scale[r : r + 1, :], (128, 128)).T
        rr = slice(128 * r, 128 * (r + 1))
        for b in range(16):
            cols = slice(128 * b, 128 * (b + 1))
            enter = jnp.where(first, seq_out[rr, cols].astype(F32), incoming[rr, cols].astype(F32))
            layer_out[rr, cols] = (enter * by * gain3[:, cols]).astype(BF)
    for batch in batches:
        batch.wait_send()

    @pl.when(c == 0)
    def _():
        relays[0].wait_send()

    @pl.when((c == 1) & (zl == 1) & (y < 3))
    def _():
        relays[1].wait_send()

    @pl.when(even_out | odd_out)
    def _():
        all_drips.wait_send()


def per_device(
    patches, patch_counts, dest_rows, qkv_weight, out_weight, attn_gain, merge_gain,
    fc1_weight, fc1_bias, fc2_weight, fc2_bias, text_embeds, section_hidden, llm_gain,
):
    vm = pl.BlockSpec(memory_space=pltpu.VMEM)
    hbm = pl.BlockSpec(memory_space=pl.ANY)
    dma = pltpu.SemaphoreType.DMA
    return pl.pallas_call(
        step_kernel,
        out_shape=[pltpu.VMEM((512, 2048), BF)] * 2,
        in_specs=[pl.BlockSpec(memory_space=pltpu.SMEM)] + [vm] * 7 + [hbm] * 6,
        out_specs=[vm] * 2,
        scratch_shapes=[
            pltpu.VMEM((3, 320, 1280), BF),
            pltpu.VMEM((320, 1280), BF),
            pltpu.VMEM((80, 1280), BF),
            pltpu.VMEM((80, 2048), BF),
            pltpu.VMEM((1, 128), jnp.int32),
            pltpu.VMEM((80, 128), BF),
            pltpu.VMEM((512, 2048), BF),
            pltpu.VMEM((512, 2048), BF),
            pltpu.VMEM((512, 2048), BF),
            pltpu.VMEM((512, 1280), BF),
            pltpu.VMEM((4, 128, 320), BF),
            pltpu.VMEM((4, 128, 320), BF),
            pltpu.VMEM((8, 2, 80, 1280), BF),
            pltpu.VMEM((16, 80, 128), BF),
            pltpu.VMEM((64, 1, 128), jnp.int32),
            pltpu.VMEM((4, 80, 128), BF),
            pltpu.VMEM((128, 1280), F32),
            pltpu.VMEM((10, 128, 128), F32),
            pltpu.VMEM((4, 32, 1280), BF),
            pltpu.VMEM((4, 4, 4, 32, 1280), BF),
            pltpu.VMEM((8, 2, 80, 1280), BF),
            pltpu.VMEM((4, 80, 512), BF),
            pltpu.VMEM((4, 4, 4, 80, 512), BF),
            pltpu.VMEM((8, 2, 16, 80, 128), BF),
            pltpu.VMEM((512, 512), F32),
            pltpu.VMEM((4, 512, 128), BF),
            pltpu.VMEM((128, 2048), BF),
            pltpu.VMEM((2048, 128), F32),
            pltpu.VMEM((64, 32, 128), BF),
            pltpu.VMEM((64, 32, 128), BF),
            pltpu.VMEM((8, 128), F32),
            pltpu.VMEM((4, 8, 128), F32),
            dma((16,)),
            dma((3 * 15 + 80 + 7,)),
            dma((5,)),
            dma((3,)),
            dma((3,)),
        ],
        compiler_params=pltpu.CompilerParams(
            collective_id=1, has_side_effects=True, vmem_limit_bytes=54 * 2**20
        ),
    )(
        patch_counts, patches, attn_gain, merge_gain, fc1_bias, fc2_bias, dest_rows, llm_gain,
        qkv_weight.transpose(1, 2, 0), out_weight, fc1_weight.T, fc2_weight,
        text_embeds, section_hidden,
    )


def solution(mesh):
    in_specs = (
        P(("section", "dp"), None),
        P(("section", "dp")),
        P(("section", "dp")),
        P(None, None, "mp"),
        P("mp", None),
        P(),
        P(),
        P("mp", ("section", "dp")),
        P(("section", "dp")),
        P(("section", "dp"), "mp"),
        P("mp"),
        P(("section", "dp"), "mp"),
        P(("section", "dp"), "mp"),
        P("mp"),
    )
    out_specs = (P(("section", "dp"), "mp"), P(("section", "dp"), "mp"))
    return jax.shard_map(
        per_device, mesh=mesh, in_specs=in_specs, out_specs=out_specs, check_vma=False
    )
```

```python
import jax
import jax.numpy as jnp
from jax import lax
from jax.experimental import pallas as pl
from jax.experimental.pallas import tpu as pltpu
from jax.sharding import PartitionSpec as P

HEAD_DIM = 80
HID = 8192
MESH = pl.DeviceIdType.MESH
BF = jnp.bfloat16
F32 = jnp.float32

vit_eps = 1e-06
llm_eps = 1e-06


def place():
    s = lax.axis_index("section")
    x = lax.axis_index("dp")
    m = lax.axis_index("mp")
    return x, s // 4, (s // 2) % 2, s % 2, m


def at(x, y, zl, c, m):
    return (y * 4 + zl * 2 + c, x, m)


class Wire:
    def __init__(self, send, recv):
        self.send, self.recv, self.sends, self.recvs = send, recv, 0, 0

    def batch(self, sent, shared=None):
        k = self.sends
        self.sends += 1
        if shared is not None:
            shared, self.recvs = self.recvs, self.recvs + 1
        return Batch(self, k, sent, shared)


class Batch:
    def __init__(self, wire, k, sent, shared):
        self.wire, self.sem, self.sent, self.shared = wire, wire.send.at[k], sent, shared

    def describe(self, src, dst, k, peer):
        return pltpu.make_async_remote_copy(
            src_ref=src, dst_ref=dst, send_sem=self.sem, recv_sem=self.wire.recv.at[k],
            device_id=peer, device_id_type=MESH,
        )

    def go(self, src, dst, peer):
        k = self.shared
        if k is None:
            k, self.wire.recvs = self.wire.recvs, self.wire.recvs + 1
        copy = self.describe(src, dst, k, peer)
        copy.start()
        self.peer = peer
        return copy

    def wait_recv(self):
        self.describe(self.sent, self.sent, self.shared, self.peer).wait_recv()

    def wait_send(self):
        self.describe(self.sent, self.sent, 0, self.peer).wait_send()


def column_gather(wire, ring_bytes, side_bytes, halves, col, column, pos, upward=(0,)):
    x, y, zl, c, m = pos
    z = 2 * m + zl
    zs = [(z + k) % 8 for k in range(8)]

    def zdev(zz, cc):
        return at(x, y, zz % 2, cc, zz // 2)

    above, below, twin = zdev(zs[1], c), zdev(zs[7], c), zdev(z, 1 - c)
    up, down = {}, {}
    up_far, down_far = upward, tuple(j for j in range(2) if j not in upward)
    ring, side = wire.batch(ring_bytes), wire.batch(side_bytes, shared=True)

    def hop(k):
        if k == 0:
            for j in range(2):
                src, dst = col.at[halves[j]], column.at[z, c].at[halves[j]]
                up[1, j] = ring.go(src, dst, above)
                down[1, j] = ring.go(src, dst, below)
            side.go(col, column.at[z, c], twin)
            return
        for j in range(2):
            for ways, z_from, peer, far in ((up, zs[8 - k], above, up_far), (down, zs[k], below, down_far)):
                if k < 4 or j in far:
                    ways[k, j].wait_recv()
                if k < 3 or (k == 3 and j in far):
                    ref = column.at[z_from, c].at[halves[j]]
                    ways[k + 1, j] = ring.go(ref, ref, peer)
        for z_from in [zs[8 - k], zs[k]][: 2 if k < 4 else 1]:
            ref = column.at[z_from, c]
            side.go(ref, ref, twin)

    return hop, side.wait_recv, [ring, side]


def shared_gather(wire, col, column, half_bytes, side_bytes, pos):
    x, y, zl, c, m = pos
    z = 2 * m + zl
    zs = [(z + k) % 8 for k in range(8)]

    def zdev(zz, cc):
        return at(x, y, zz % 2, cc, zz // 2)

    above, below, twin = zdev(zs[1], c), zdev(zs[7], c), zdev(z, 1 - c)
    right, left = at((x + 1) % 4, y, zl, c, m), at((x + 3) % 4, y, zl, c, m)
    mine = pl.ds(pl.multiple_of((x % 2) * 640, 128), 640)
    other = pl.ds(pl.multiple_of((1 - x % 2) * 640, 128), 640)
    ring, across = wire.batch(half_bytes), wire.batch(half_bytes)
    side = wire.batch(side_bytes, shared=True)
    ways = {}
    crossed = []

    def hop(k):
        if k == 0:
            dst = column.at[z, c].at[:, mine]
            ways["up", 1] = ring.go(col.at[:, mine], dst, above)
            ways["down", 1] = ring.go(col.at[:, mine], dst, below)
            side.go(col, column.at[z, c], twin)
            return
        for way, z_from, peer, beside, end in (
            ("up", zs[8 - k], above, right, 4), ("down", zs[k], below, left, 3)
        ):
            if k <= end:
                ways[way, k].wait_recv()
                ref = column.at[z_from, c].at[:, mine]
                if k < end:
                    ways[way, k + 1] = ring.go(ref, ref, peer)
                crossed.append((across.go(ref, ref, beside), column.at[z_from, c].at[:, other]))
                side.go(ref, ref, twin)

    def finish():
        for copy, ref in crossed:
            copy.wait_recv()
            side.go(ref, ref, twin)
        side.wait_recv()

    return hop, finish, [ring, across, side]


def plane_gather(cp, blk, plane, points, pos):
    x, y, zl, c, m = pos
    xs = [(x + k) % 4 for k in range(4)]
    ys = [(y + k) % 4 for k in range(4)]
    right, left = at(xs[1], y, zl, c, m), at(xs[3], y, zl, c, m)
    up, down = at(x, ys[1], zl, c, m), at(x, ys[3], zl, c, m)
    ahead = [[(right, left), (up, down)], [(up, down), (right, left)]]

    def block(v, a, b, lo, hi):
        fx, fy = (xs[a], ys[b]) if v == 0 else (xs[b], ys[a])
        return plane.at[2 * v + lo : 2 * v + hi, fy, fx]

    def push(v, axis, sgn, a, b, lo=0, hi=2, own=False):
        src = blk.at[2 * v + lo : 2 * v + hi] if own else block(v, a, b, lo, hi)
        return cp.go(src, block(v, a, b, lo, hi), ahead[v][axis][0 if sgn > 0 else 1])

    one, two, three, four = {}, {}, {}, {}
    for v in range(2):
        for g in (1, -1):
            one[v, g] = push(v, 0, g, 0, 0, own=True)
    for v in range(2):
        for g in (1, -1):
            three[v, 0, g] = push(v, 1, g, 0, 0, own=True)
    points[0]()
    plane[:, y, x] = blk[...]
    for g in (1, -1):
        for v in range(2):
            one[v, g].wait_recv()
            a = -g % 4
            two[v, g] = push(v, 0, g, a, 0, *((0, 1) if g > 0 else (1, 2)))
            for h in (1, -1):
                three[v, a, h] = push(v, 1, h, a, 0)
    points[1]()

    def opposite(a):
        for g in (1, -1):
            for v in range(2):
                three[v, a, g].wait_recv()
                four[v, a, g] = push(v, 1, g, a, -g % 4, *((0, 1) if g > 0 else (1, 2)))

    opposite(0)
    for v in range(2):
        for g in (1, -1):
            two[v, g].wait_recv()
        for h in (1, -1):
            three[v, 2, h] = push(v, 1, h, 2, 0)
    points[2]()
    opposite(3)
    opposite(1)
    points[3]()
    opposite(2)
    points[4]()
    for copy in four.values():
        copy.wait_recv()


BY_ROWS = (slice(0, 48), slice(48, 80))
NT = (((1,), (1,)), ((), ()))
TN = (((0,), (0,)), ((), ()))


def dot(a, b, dims=(((1,), (0,)), ((), ()))):
    return lax.dot_general(a, b, dims, preferred_element_type=F32)


def normed(v, gain):
    v = v - jnp.mean(v, axis=-1, keepdims=True)
    return v * lax.rsqrt(jnp.mean(v * v, axis=-1, keepdims=True) + vit_eps) * gain


def step_kernel(
    counts, patches, attn_gain, merge_gain, fc1_bias, fc2_bias, dest_rows, llm_gain,
    wqkv_hbm, wout_hbm, fc1_hbm, fc2_hbm, text_hbm, hidden_hbm,
    seq_out, layer_out,
    wqkv, wout, fc1, fc2, dest, bias1,
    text, incoming, stage,
    xn, att, attr, wout_all, f2p, dall, ball, nrm, turn, blk1, rows_all, fc1_all,
    blk2, hid_all, fc2_all, acc1, acc, second, mid, emb, flat, send_rows, got, sq_own, sq_all,
    send, recv, local, relay_send, relay_recv,
):
    pos = place()
    x, y, zl, c, m = pos
    s = y * 4 + zl * 2 + c
    z = 2 * m + zl
    mine = y * 4 + x
    note = (zl * 2 + c) * 16 + mine
    across = [(s, x, (m + k) % 4) for k in (2, 1, 3)]
    groups = [((s + i) % 16, (x + j) % 4, m) for i in range(16) for j in range(4) if i or j]
    barrier = pltpu.get_barrier_semaphore()
    column = [at(x, y, 1 - zl, c, (m + 1) % 4), at(x, y, 1 - zl, c, (m + 3) % 4)]
    peers = across + groups + column
    for peer in peers:
        pl.semaphore_signal(barrier, inc=1, device_id=peer, device_id_type=MESH)

    loads = [
        pltpu.make_async_copy(a, b, local.at[k])
        for k, (a, b) in enumerate(
            ((wout_hbm, wout), (fc2_hbm, fc2), (wqkv_hbm, wqkv), (fc1_hbm, fc1), (text_hbm, text))
        )
    ]
    for copy in loads:
        copy.start()

    pl.semaphore_wait(barrier, len(peers))

    wire = Wire(send, recv)
    relay_to = [at(x, y, zl, 1, m), at(x, (y + 1) % 4, 1, 0, m), at(x, y, 1 - zl, 0, m)]
    relays = [
        pltpu.make_async_remote_copy(
            src_ref=hidden_hbm, dst_ref=ref, send_sem=relay_send.at[k], recv_sem=relay_recv.at[k],
            device_id=relay_to[k], device_id_type=MESH,
        )
        for k, ref in ((0, incoming), (1, stage))
    ]
    even_out, odd_out = (c == 1) & (zl == 0), (c == 0) & (zl == 1) & (y > 0)
    drips = []
    for k in range(16):
        r = slice(32 * k, 32 * (k + 1))
        drips.append(
            [
                pltpu.make_async_remote_copy(
                    src_ref=ref.at[r], dst_ref=incoming.at[r],
                    send_sem=relay_send.at[2], recv_sem=relay_recv.at[2],
                    device_id=relay_to[2], device_id_type=MESH,
                )
                for ref in (hidden_hbm, stage)
            ]
        )
    all_drips = pltpu.make_async_remote_copy(
        src_ref=stage, dst_ref=incoming, send_sem=relay_send.at[2], recv_sem=relay_recv.at[2],
        device_id=relay_to[2], device_id_type=MESH,
    )

    def drip(k):
        for j in range((0, 3, 6, 9, 11, 13, 15, 16, 16)[k], (3, 6, 9, 11, 13, 15, 16, 16, 16)[k]):

            @pl.when(even_out)
            def _():
                drips[j][0].start()

            @pl.when(odd_out)
            def _():
                drips[j][1].start()

    loads[0].wait()
    half_rows = pl.ds(pl.multiple_of((zl * 2 + c) * 80, 16), 80)
    hop0, finish0, batches = shared_gather(
        wire, wout.at[half_rows], wout_all, fc1_all.at[0:7, 0, :, 0:640], fc1_all.at[0:4], pos
    )
    hop0(0)

    @pl.when((c == 1) & (zl == 1) & (y < 3))
    def _():
        relays[1].start()

    @pl.when(c == 0)
    def _():
        relays[0].start()

    loads[1].wait()
    pieces = wire.batch(f2p.at[0:15], shared=True)
    notes = wire.batch(dall.at[0:63], shared=True)
    biases = wire.batch(ball.at[0:3], shared=True)
    parts = wire.batch(attr.at[0:3], shared=True)
    batches += [pieces, notes, biases, parts]
    for dy in range(4):
        for dx in range(4):
            if dx or dy:
                px, py = (x + dx) % 4, (y + dy) % 4
                cols = pl.ds(pl.multiple_of((py * 4 + px) * 128, 128), 128)
                pieces.go(fc2.at[:, cols], f2p.at[mine], at(px, py, zl, c, m))
    j_lane = lax.broadcasted_iota(jnp.int32, (1, 128), 1)
    dest_row = dest_rows[...].reshape(1, 128)
    tile_count = jnp.where(j_lane < 64, counts[0], counts[1])
    live = (j_lane % 64) * 4 < tile_count
    dest[...] = jnp.where(live, dest_row, 2**30)
    bias_row = fc1_bias[...].reshape(1, 80)
    top = lax.broadcasted_iota(jnp.int32, (8, 80), 0) == 0
    bias_row = jnp.where(top, bias_row.astype(F32), 0.0).astype(BF)
    bias1[...] = dot(bias_row, jnp.ones((8, 128), BF), TN).astype(BF)
    k_lane = lax.broadcasted_iota(jnp.int32, (1, 256), 1)
    key_bias = [jnp.where(k_lane < counts[t], 0.0, -1e30) for t in range(2)]

    for peer in groups:
        notes.go(dest, dall.at[note], peer)
    for dz in range(2):
        for dc in range(2):
            if dz or dc:
                biases.go(bias1, ball.at[zl * 2 + c], at(x, y, (zl + dz) % 2, (c + dc) % 2, m))
    f2p[mine] = fc2[:, pl.ds(pl.multiple_of(mine * 128, 128), 128)]
    dall[note] = dest[...]
    ball[zl * 2 + c] = bias1[...]
    wout_all[z, c] = wout[half_rows, :]
    loads[2].wait()

    gain1 = attn_gain[...].reshape(1, 1280).astype(F32)

    def norm_rows(i, carry):
        r = pl.ds(pl.multiple_of(i * 32, 32), 32)
        xn[r, :] = normed(patches[r, :].astype(F32), gain1).astype(BF)
        return carry

    lax.fori_loop(0, 16, norm_rows, 0)

    hop0(1)
    lane = lax.broadcasted_iota(jnp.int32, (256, 320), 1)
    for t in range(2):
        xt = xn[256 * t : 256 * (t + 1), :]
        q, k, v = (dot(xt, wqkv[j], NT).astype(BF) for j in range(3))
        out = jnp.zeros((256, 320), F32)
        for h in range(4):
            inside = (lane >= 80 * h) & (lane < 80 * (h + 1))
            sc = dot(jnp.where(inside, q, jnp.zeros_like(q)), k, NT) * HEAD_DIM ** (-0.5)
            sc = sc + key_bias[t]
            sc = jnp.exp(sc - jnp.max(sc, axis=1, keepdims=True))
            w = (sc / jnp.sum(sc, axis=1, keepdims=True)).astype(BF)
            out = jnp.where(inside, dot(w, v), out)
        att[2 * t : 2 * t + 2] = out.astype(BF).reshape(2, 128, 320)
    hop0(2)
    for peer in across:
        parts.go(att.at[peer[2]], attr.at[m], peer)
    attr[m] = att[m]
    for k in range(3, 5):
        hop0(k)
    finish0()
    parts.wait_recv()
    for k in range(4):
        w = wout_all[2 * k : 2 * k + 2].reshape(320, 1280)
        part = dot(attr[k], w)
        nrm[...] = part if k == 0 else nrm[...] + part
    gain2 = merge_gain[...].reshape(1, 1280).astype(F32)
    for i in range(4):
        r = pl.ds(pl.multiple_of(m * 128 + 32 * i, 32), 32)
        o = (patches[r, :].astype(F32) + nrm[32 * i : 32 * (i + 1), :]).astype(BF)
        o = normed(o.astype(F32), gain2)
        for b in range(10):
            turn[b, 32 * i : 32 * (i + 1), :] = o[:, 128 * b : 128 * (b + 1)]
    for p in range(4):
        for b in range(10):
            cols = slice(128 * b, 128 * (b + 1))
            blk1[p, :, cols] = turn[b, pl.ds(p, 32, stride=4), :].astype(BF)

    loads[3].wait()

    @pl.when(odd_out)
    def _():
        relays[1].wait_recv()

    hop1, finish1, more = column_gather(
        wire, fc1_all.at[0:7, 0], fc1_all.at[0:4], BY_ROWS, fc1, fc1_all, pos
    )
    planes = [wire.batch(fc2_all.at[:, :, 0:15]) for _ in range(2)]
    batches += more + planes
    fc1_all[z, c] = fc1[...]

    def point(*calls):
        def run():
            for call, k in calls:
                call(k)

        return run

    pieces.wait_recv()
    hop2, finish2, more = column_gather(
        wire, fc2_all.at[0:7, 0], fc2_all.at[0:4], (slice(0, 8), slice(8, 16)), f2p, fc2_all, pos
    )
    batches += more
    fc2_all[z, c] = f2p[...]
    plane_gather(
        planes[0],
        blk1,
        rows_all,
        [
            point((hop1, 0)),
            point((hop1, 1), (drip, 0)),
            point((hop1, 2), (drip, 1)),
            point((hop1, 3), (drip, 2)),
            point((hop1, 4), (hop2, 0), (drip, 3)),
        ],
        pos,
    )
    finish1()
    biases.wait_recv()
    for p in range(4):
        part = dot(
            fc1_all[2 * p : 2 * p + 2].reshape(320, 1280), rows_all[p].reshape(512, 1280), NT
        )
        acc1[...] = part if p == 0 else acc1[...] + part
    for b in range(4):
        h = acc1[80 * b : 80 * (b + 1), :] + ball[b][:, :1].astype(F32)
        blk2[b] = (0.5 * h * (1.0 + lax.erf(h * 0.5**0.5))).astype(BF)

    plane_gather(
        planes[1],
        blk2,
        hid_all,
        [
            point(),
            point((hop2, 1), (drip, 4)),
            point((hop2, 2), (drip, 5)),
            point((hop2, 3), (drip, 6)),
            point((hop2, 4), (drip, 7)),
        ],
        pos,
    )
    finish2()

    direct = wire.batch(emb.at[0:2], shared=True)
    halfway = wire.batch(emb.at[0])
    onward = wire.batch(emb.at[0], shared=True)
    picked = wire.batch(got.at[0:63], shared=True)
    sums = wire.batch(sq_all.at[0:3], shared=True)
    batches += [direct, halfway, onward, picked, sums]
    ms = [(m + k) % 4 for k in range(4)]
    upper, lower = slice(0, 256), slice(256, 512)
    via = []
    for half in range(2):
        r = (upper, lower)[half]
        for b in range(4):
            w = jnp.concatenate(
                [fc2_all[2 * k + b // 2, b % 2].reshape(1280, 128) for k in range(4)], axis=1
            )
            part = dot(hid_all[b, :, :, :, r].reshape(1280, 256), w, TN)
            acc[...] = part if b == 0 else acc[...] + part
        for k in range(4):
            second[k, r, :] = acc[:, 128 * k : 128 * (k + 1)].astype(BF)
        via.append(halfway.go(second.at[ms[2], r], mid.at[half], across[1 + half]))
        for k in (1, 3):
            direct.go(second.at[ms[k], r], emb.at[m, r], across[1 + k // 2])
    emb[m] = second[m]
    for half in range(2):
        via[half].wait_recv()
        r = (upper, lower)[half]
        onward.go(mid.at[half], emb.at[ms[3 - 2 * half], r], across[1 + half])
    notes.wait_recv()
    near = dall[pl.ds(pl.multiple_of((zl * 2 + c) * 16, 16), 16)]
    receiver = lax.broadcasted_iota(jnp.int32, (64, 128), 0)
    odd = lax.broadcasted_iota(jnp.int32, (64, 128), 1) % 2
    bias2 = fc2_bias[...].reshape(1, 2048).astype(F32)
    own_bias = jnp.zeros((1, 128), F32)
    for b in range(16):
        own_bias = jnp.where(mine == b, bias2[:, 128 * b : 128 * (b + 1)], own_bias)
    direct.wait_recv()
    onward.wait_recv()
    for q in range(16):
        e = emb[:, 32 * q : 32 * (q + 1), :].reshape(128, 128)
        e = (e.astype(F32) + own_bias).astype(BF)
        to_here = receiver == near[q] // 512
        for i in range(2):
            pick = (to_here & (odd == i)).astype(F32).astype(BF)
            flat[pl.ds(2 * q + i, 64, stride=32), :] = dot(pick, e)
    send_rows[...] = flat[...].astype(BF).reshape(64, 32, 128)
    for peer in groups:
        picked.go(send_rows.at[peer[0] * 4 + peer[1]], got.at[s * 4 + x], peer)
    drip(8)
    got[s * 4 + x] = send_rows[s * 4 + x]
    d = dall[...].reshape(64, 128)
    low = (s * 4 + x) * 512
    row = lax.broadcasted_iota(jnp.int32, (64, 512), 1)
    here = (d >= low) & (d < low + 512)
    puts = []
    for i in range(2):
        spot = jnp.max(jnp.where(here & (odd == i), (d - low).astype(F32), -1.0), axis=1, keepdims=True)
        puts.append((row == spot.astype(jnp.int32)).astype(F32).astype(BF))
    loads[4].wait()

    @pl.when(c == 1)
    def _():
        relays[0].wait_recv()

    @pl.when((c == 0) & (s > 0))
    def _():
        all_drips.wait_recv()

    picked.wait_recv()
    flat[...] = got[...].reshape(2048, 128).astype(F32)
    ones = jnp.ones((64, 128), BF)
    first = s == 0
    squares = [jnp.zeros((128, 128), F32) for _ in range(4)]
    hits = [
        dot(puts[0][:, 128 * r : 128 * (r + 1)], ones, TN)
        + dot(puts[1][:, 128 * r : 128 * (r + 1)], ones, TN)
        for r in range(4)
    ]
    for b in range(16):
        new = [
            jnp.concatenate(
                [
                    flat[pl.ds(((b // 4 * 4 + zc) * 4 + b % 4) * 32 + i, 16, stride=2), :]
                    for zc in range(4)
                ],
                axis=0,
            ).astype(BF)
            for i in range(2)
        ]
        cols = slice(128 * b, 128 * (b + 1))
        for r in range(4):
            rr = slice(128 * r, 128 * (r + 1))
            placed = dot(puts[0][:, rr], new[0], TN) + dot(puts[1][:, rr], new[1], TN)
            seq = jnp.where(hits[r] > 0.5, placed, text[rr, cols].astype(F32))
            seq_out[rr, cols] = seq.astype(BF)
            enter = jnp.where(first, seq, incoming[rr, cols].astype(F32))
            squares[r] = squares[r] + enter * enter
    sub = lax.broadcasted_iota(jnp.int32, (8, 128), 0)
    total = jnp.zeros((8, 128), F32)
    for r in range(4):
        line = jnp.broadcast_to(jnp.sum(squares[r], axis=1, keepdims=True), (128, 128)).T
        total = jnp.where(sub == r, line[0:8], total)
    sq_own[...] = total
    for peer in across:
        sums.go(sq_own, sq_all.at[m], peer)
    sq_all[m] = total
    sums.wait_recv()
    total = (sq_all[0] + sq_all[1]) + (sq_all[2] + sq_all[3])
    scale = lax.rsqrt(total / HID + llm_eps)
    gain3 = llm_gain[...].reshape(1, 2048).astype(F32)
    for r in range(4):
        by = jnp.broadcast_to(scale[r : r + 1, :], (128, 128)).T
        rr = slice(128 * r, 128 * (r + 1))
        for b in range(16):
            cols = slice(128 * b, 128 * (b + 1))
            enter = jnp.where(first, seq_out[rr, cols].astype(F32), incoming[rr, cols].astype(F32))
            layer_out[rr, cols] = (enter * by * gain3[:, cols]).astype(BF)
    for batch in batches:
        batch.wait_send()

    @pl.when(c == 0)
    def _():
        relays[0].wait_send()

    @pl.when((c == 1) & (zl == 1) & (y < 3))
    def _():
        relays[1].wait_send()

    @pl.when(even_out | odd_out)
    def _():
        all_drips.wait_send()


def per_device(
    patches, patch_counts, dest_rows, qkv_weight, out_weight, attn_gain, merge_gain,
    fc1_weight, fc1_bias, fc2_weight, fc2_bias, text_embeds, section_hidden, llm_gain,
):
    vm = pl.BlockSpec(memory_space=pltpu.VMEM)
    hbm = pl.BlockSpec(memory_space=pl.ANY)
    dma = pltpu.SemaphoreType.DMA
    return pl.pallas_call(
        step_kernel,
        out_shape=[pltpu.VMEM((512, 2048), BF)] * 2,
        in_specs=[pl.BlockSpec(memory_space=pltpu.SMEM)] + [vm] * 7 + [hbm] * 6,
        out_specs=[vm] * 2,
        scratch_shapes=[
            pltpu.VMEM((3, 320, 1280), BF),
            pltpu.VMEM((320, 1280), BF),
            pltpu.VMEM((80, 1280), BF),
            pltpu.VMEM((80, 2048), BF),
            pltpu.VMEM((1, 128), jnp.int32),
            pltpu.VMEM((80, 128), BF),
            pltpu.VMEM((512, 2048), BF),
            pltpu.VMEM((512, 2048), BF),
            pltpu.VMEM((512, 2048), BF),
            pltpu.VMEM((512, 1280), BF),
            pltpu.VMEM((4, 128, 320), BF),
            pltpu.VMEM((4, 128, 320), BF),
            pltpu.VMEM((8, 2, 80, 1280), BF),
            pltpu.VMEM((16, 80, 128), BF),
            pltpu.VMEM((64, 1, 128), jnp.int32),
            pltpu.VMEM((4, 80, 128), BF),
            pltpu.VMEM((128, 1280), F32),
            pltpu.VMEM((10, 128, 128), F32),
            pltpu.VMEM((4, 32, 1280), BF),
            pltpu.VMEM((4, 4, 4, 32, 1280), BF),
            pltpu.VMEM((8, 2, 80, 1280), BF),
            pltpu.VMEM((4, 80, 512), BF),
            pltpu.VMEM((4, 4, 4, 80, 512), BF),
            pltpu.VMEM((8, 2, 16, 80, 128), BF),
            pltpu.VMEM((320, 512), F32),
            pltpu.VMEM((256, 512), F32),
            pltpu.VMEM((4, 512, 128), BF),
            pltpu.VMEM((2, 256, 128), BF),
            pltpu.VMEM((4, 512, 128), BF),
            pltpu.VMEM((2048, 128), F32),
            pltpu.VMEM((64, 32, 128), BF),
            pltpu.VMEM((64, 32, 128), BF),
            pltpu.VMEM((8, 128), F32),
            pltpu.VMEM((4, 8, 128), F32),
            dma((18,)),
            dma((3 * 15 + 80 + 10,)),
            dma((5,)),
            dma((3,)),
            dma((3,)),
        ],
        compiler_params=pltpu.CompilerParams(
            collective_id=1, has_side_effects=True, vmem_limit_bytes=54 * 2**20
        ),
    )(
        patch_counts, patches, attn_gain, merge_gain, fc1_bias, fc2_bias, dest_rows, llm_gain,
        qkv_weight.transpose(1, 2, 0), out_weight, fc1_weight.T, fc2_weight,
        text_embeds, section_hidden,
    )


def solution(mesh):
    in_specs = (
        P(("section", "dp"), None),
        P(("section", "dp")),
        P(("section", "dp")),
        P(None, None, "mp"),
        P("mp", None),
        P(),
        P(),
        P("mp", ("section", "dp")),
        P(("section", "dp")),
        P(("section", "dp"), "mp"),
        P("mp"),
        P(("section", "dp"), "mp"),
        P(("section", "dp"), "mp"),
        P("mp"),
    )
    out_specs = (P(("section", "dp"), "mp"), P(("section", "dp"), "mp"))
    return jax.shard_map(
        per_device, mesh=mesh, in_specs=in_specs, out_specs=out_specs, check_vma=False
    )
```

```python
import jax
import jax.numpy as jnp
from jax import lax
from jax.experimental import pallas as pl
from jax.experimental.pallas import tpu as pltpu
from jax.sharding import PartitionSpec as P

HEAD_DIM = 80
HID = 8192
MESH = pl.DeviceIdType.MESH
BF = jnp.bfloat16
F32 = jnp.float32

vit_eps = 1e-06
llm_eps = 1e-06


def place():
    s = lax.axis_index("section")
    x = lax.axis_index("dp")
    m = lax.axis_index("mp")
    return x, s // 4, (s // 2) % 2, s % 2, m


def at(x, y, zl, c, m):
    return (y * 4 + zl * 2 + c, x, m)


class Wire:
    def __init__(self, send, recv):
        self.send, self.recv, self.sends, self.recvs = send, recv, 0, 0

    def batch(self, sent, shared=None):
        k = self.sends
        self.sends += 1
        if shared is not None:
            shared, self.recvs = self.recvs, self.recvs + 1
        return Batch(self, k, sent, shared)


class Batch:
    def __init__(self, wire, k, sent, shared):
        self.wire, self.sem, self.sent, self.shared = wire, wire.send.at[k], sent, shared

    def describe(self, src, dst, k, peer):
        return pltpu.make_async_remote_copy(
            src_ref=src, dst_ref=dst, send_sem=self.sem, recv_sem=self.wire.recv.at[k],
            device_id=peer, device_id_type=MESH,
        )

    def go(self, src, dst, peer):
        k = self.shared
        if k is None:
            k, self.wire.recvs = self.wire.recvs, self.wire.recvs + 1
        copy = self.describe(src, dst, k, peer)
        copy.start()
        self.peer = peer
        return copy

    def wait_recv(self):
        self.describe(self.sent, self.sent, self.shared, self.peer).wait_recv()

    def wait_send(self):
        self.describe(self.sent, self.sent, 0, self.peer).wait_send()


def column_gather(wire, ring_bytes, side_bytes, halves, col, column, pos, upward=(0,)):
    x, y, zl, c, m = pos
    z = 2 * m + zl
    zs = [(z + k) % 8 for k in range(8)]

    def zdev(zz, cc):
        return at(x, y, zz % 2, cc, zz // 2)

    above, below, twin = zdev(zs[1], c), zdev(zs[7], c), zdev(z, 1 - c)
    up, down = {}, {}
    up_far, down_far = upward, tuple(j for j in range(2) if j not in upward)
    ring, side = wire.batch(ring_bytes), wire.batch(side_bytes, shared=True)

    def hop(k):
        if k == 0:
            for j in range(2):
                src, dst = col.at[halves[j]], column.at[z, c].at[halves[j]]
                up[1, j] = ring.go(src, dst, above)
                down[1, j] = ring.go(src, dst, below)
            side.go(col, column.at[z, c], twin)
            return
        for j in range(2):
            for ways, z_from, peer, far in ((up, zs[8 - k], above, up_far), (down, zs[k], below, down_far)):
                if k < 4 or j in far:
                    ways[k, j].wait_recv()
                if k < 3 or (k == 3 and j in far):
                    ref = column.at[z_from, c].at[halves[j]]
                    ways[k + 1, j] = ring.go(ref, ref, peer)
        for z_from in [zs[8 - k], zs[k]][: 2 if k < 4 else 1]:
            ref = column.at[z_from, c]
            side.go(ref, ref, twin)

    return hop, side.wait_recv, [ring, side]


def shared_gather(wire, col, column, half_bytes, side_bytes, pos):
    x, y, zl, c, m = pos
    z = 2 * m + zl
    zs = [(z + k) % 8 for k in range(8)]

    def zdev(zz, cc):
        return at(x, y, zz % 2, cc, zz // 2)

    above, below, twin = zdev(zs[1], c), zdev(zs[7], c), zdev(z, 1 - c)
    right, left = at((x + 1) % 4, y, zl, c, m), at((x + 3) % 4, y, zl, c, m)
    mine = pl.ds(pl.multiple_of((x % 2) * 640, 128), 640)
    other = pl.ds(pl.multiple_of((1 - x % 2) * 640, 128), 640)
    ring, across = wire.batch(half_bytes), wire.batch(half_bytes)
    side = wire.batch(side_bytes, shared=True)
    ways = {}
    crossed = []

    def hop(k):
        if k == 0:
            dst = column.at[z, c].at[:, mine]
            ways["up", 1] = ring.go(col.at[:, mine], dst, above)
            ways["down", 1] = ring.go(col.at[:, mine], dst, below)
            side.go(col, column.at[z, c], twin)
            return
        for way, z_from, peer, beside, end in (
            ("up", zs[8 - k], above, right, 4), ("down", zs[k], below, left, 3)
        ):
            if k <= end:
                ways[way, k].wait_recv()
                ref = column.at[z_from, c].at[:, mine]
                if k < end:
                    ways[way, k + 1] = ring.go(ref, ref, peer)
                crossed.append((across.go(ref, ref, beside), column.at[z_from, c].at[:, other]))
                side.go(ref, ref, twin)

    def finish():
        for copy, ref in crossed:
            copy.wait_recv()
            side.go(ref, ref, twin)
        side.wait_recv()

    return hop, finish, [ring, across, side]


def plane_gather(cp, blk, plane, points, pos):
    x, y, zl, c, m = pos
    xs = [(x + k) % 4 for k in range(4)]
    ys = [(y + k) % 4 for k in range(4)]
    right, left = at(xs[1], y, zl, c, m), at(xs[3], y, zl, c, m)
    up, down = at(x, ys[1], zl, c, m), at(x, ys[3], zl, c, m)
    ahead = [[(right, left), (up, down)], [(up, down), (right, left)]]

    def block(v, a, b, lo, hi):
        fx, fy = (xs[a], ys[b]) if v == 0 else (xs[b], ys[a])
        return plane.at[2 * v + lo : 2 * v + hi, fy, fx]

    def push(v, axis, sgn, a, b, lo=0, hi=2, own=False):
        src = blk.at[2 * v + lo : 2 * v + hi] if own else block(v, a, b, lo, hi)
        return cp.go(src, block(v, a, b, lo, hi), ahead[v][axis][0 if sgn > 0 else 1])

    one, two, three, four = {}, {}, {}, {}
    for v in range(2):
        for g in (1, -1):
            one[v, g] = push(v, 0, g, 0, 0, own=True)
    for v in range(2):
        for g in (1, -1):
            three[v, 0, g] = push(v, 1, g, 0, 0, own=True)
    points[0]()
    plane[:, y, x] = blk[...]
    for g in (1, -1):
        for v in range(2):
            one[v, g].wait_recv()
            a = -g % 4
            two[v, g] = push(v, 0, g, a, 0, *((0, 1) if g > 0 else (1, 2)))
            for h in (1, -1):
                three[v, a, h] = push(v, 1, h, a, 0)
    points[1]()

    def opposite(a, between=None):
        for g in (1, -1):
            for v in range(2):
                three[v, a, g].wait_recv()
                four[v, a, g] = push(v, 1, g, a, -g % 4, *((0, 1) if g > 0 else (1, 2)))
            if between is not None and g == 1:
                between()

    opposite(0, points[2])
    for v in range(2):
        for g in (1, -1):
            two[v, g].wait_recv()
        for h in (1, -1):
            three[v, 2, h] = push(v, 1, h, 2, 0)
    points[3]()
    opposite(3)
    opposite(1)
    points[4]()
    opposite(2)
    points[5]()
    for copy in four.values():
        copy.wait_recv()


BY_ROWS = (slice(0, 48), slice(48, 80))
NT = (((1,), (1,)), ((), ()))
TN = (((0,), (0,)), ((), ()))


def dot(a, b, dims=(((1,), (0,)), ((), ()))):
    return lax.dot_general(a, b, dims, preferred_element_type=F32)


def normed(v, gain):
    v = v - jnp.mean(v, axis=-1, keepdims=True)
    return v * lax.rsqrt(jnp.mean(v * v, axis=-1, keepdims=True) + vit_eps) * gain


def step_kernel(
    counts, patches, attn_gain, merge_gain, fc1_bias, fc2_bias, dest_rows, llm_gain,
    wqkv_hbm, wout_hbm, fc1_hbm, fc2_hbm, text_hbm, hidden_hbm,
    seq_out, layer_out,
    wqkv, wout, fc1, fc2, dest, bias1,
    text, incoming, stage,
    xn, att, att_mid, attr, wout_all, f2p, dall, ball, nrm, turn, blk1, rows_all, fc1_all,
    blk2, hid_all, fc2_all, acc1, acc, second, mid, emb, flat, send_rows, got, sq_own, sq_all,
    send, recv, local, relay_send, relay_recv,
):
    pos = place()
    x, y, zl, c, m = pos
    s = y * 4 + zl * 2 + c
    z = 2 * m + zl
    mine = y * 4 + x
    note = (zl * 2 + c) * 16 + mine
    across = [(s, x, (m + k) % 4) for k in (2, 1, 3)]
    groups = [((s + i) % 16, (x + j) % 4, m) for i in range(16) for j in range(4) if i or j]
    barrier = pltpu.get_barrier_semaphore()
    column = [at(x, y, 1 - zl, c, (m + 1) % 4), at(x, y, 1 - zl, c, (m + 3) % 4)]
    peers = across + groups + column
    for peer in peers:
        pl.semaphore_signal(barrier, inc=1, device_id=peer, device_id_type=MESH)

    loads = [
        pltpu.make_async_copy(a, b, local.at[k])
        for k, (a, b) in enumerate(
            ((wout_hbm, wout), (fc2_hbm, fc2), (wqkv_hbm, wqkv), (fc1_hbm, fc1), (text_hbm, text))
        )
    ]
    for copy in loads:
        copy.start()

    pl.semaphore_wait(barrier, len(peers))

    wire = Wire(send, recv)
    relay_to = [at(x, y, zl, 1, m), at(x, (y + 1) % 4, 1, 0, m), at(x, y, 1 - zl, 0, m)]
    relays = [
        pltpu.make_async_remote_copy(
            src_ref=src, dst_ref=ref, send_sem=relay_send.at[k], recv_sem=relay_recv.at[k],
            device_id=relay_to[k], device_id_type=MESH,
        )
        for k, src, ref in ((0, hidden_hbm, incoming), (1, hidden_hbm.at[256:512], stage))
    ]
    early_out = (c == 1) & (s < 15)
    earlies = [
        pltpu.make_async_remote_copy(
            src_ref=hidden_hbm.at[32 * k : 32 * (k + 1)],
            dst_ref=incoming.at[32 * k : 32 * (k + 1)],
            send_sem=relay_send.at[3], recv_sem=relay_recv.at[2],
            device_id=((s + 1) % 16, x, m), device_id_type=MESH,
        )
        for k in range(8)
    ]

    def early(lo, hi):
        @pl.when(early_out)
        def _():
            for k in range(lo, hi):
                earlies[k].start()

    even_out, odd_out = (c == 1) & (zl == 0), (c == 0) & (zl == 1) & (y > 0)
    drips = []
    for k in range(8):
        r, r_stage = (slice(32 * k + low, 32 * (k + 1) + low) for low in (256, 0))
        drips.append(
            [
                pltpu.make_async_remote_copy(
                    src_ref=ref, dst_ref=incoming.at[r],
                    send_sem=relay_send.at[2], recv_sem=relay_recv.at[2],
                    device_id=relay_to[2], device_id_type=MESH,
                )
                for ref in (hidden_hbm.at[r], stage.at[r_stage])
            ]
        )
    all_in = pltpu.make_async_remote_copy(
        src_ref=incoming, dst_ref=incoming, send_sem=relay_send.at[2], recv_sem=relay_recv.at[2],
        device_id=relay_to[2], device_id_type=MESH,
    )
    drips_out, earlies_out = (
        pltpu.make_async_remote_copy(
            src_ref=stage, dst_ref=stage, send_sem=relay_send.at[k], recv_sem=relay_recv.at[2],
            device_id=relay_to[2], device_id_type=MESH,
        )
        for k in (2, 3)
    )

    def drip(k):
        for j in range((0, 2, 4, 5, 6, 7, 8, 8)[k], (2, 4, 5, 6, 7, 8, 8, 8)[k]):

            @pl.when(even_out)
            def _():
                drips[j][0].start()

            @pl.when(odd_out)
            def _():
                drips[j][1].start()

    loads[0].wait()
    half_rows = pl.ds(pl.multiple_of((zl * 2 + c) * 80, 16), 80)
    hop0, finish0, batches = shared_gather(
        wire, wout.at[half_rows], wout_all, fc1_all.at[0:7, 0, :, 0:640], fc1_all.at[0:4], pos
    )
    hop0(0)

    @pl.when((c == 1) & (zl == 1) & (y < 3))
    def _():
        relays[1].start()

    @pl.when(c == 0)
    def _():
        relays[0].start()

    early(0, 3)

    loads[1].wait()
    pieces = wire.batch(f2p.at[0:15], shared=True)
    notes = wire.batch(dall.at[0:63], shared=True)
    biases = wire.batch(ball.at[0:3], shared=True)
    parts = wire.batch(attr.at[0:2], shared=True)
    parts_by, parts_on = wire.batch(attr.at[0]), wire.batch(attr.at[0], shared=True)
    batches += [pieces, notes, biases, parts, parts_by, parts_on]
    for dy in range(4):
        for dx in range(4):
            if dx or dy:
                px, py = (x + dx) % 4, (y + dy) % 4
                cols = pl.ds(pl.multiple_of((py * 4 + px) * 128, 128), 128)
                pieces.go(fc2.at[:, cols], f2p.at[mine], at(px, py, zl, c, m))
    j_lane = lax.broadcasted_iota(jnp.int32, (1, 128), 1)
    dest_row = dest_rows[...].reshape(1, 128)
    tile_count = jnp.where(j_lane < 64, counts[0], counts[1])
    live = (j_lane % 64) * 4 < tile_count
    dest[...] = jnp.where(live, dest_row, 2**30)
    bias_row = fc1_bias[...].reshape(1, 80)
    top = lax.broadcasted_iota(jnp.int32, (8, 80), 0) == 0
    bias_row = jnp.where(top, bias_row.astype(F32), 0.0).astype(BF)
    bias1[...] = dot(bias_row, jnp.ones((8, 128), BF), TN).astype(BF)
    k_lane = lax.broadcasted_iota(jnp.int32, (1, 256), 1)
    key_bias = [jnp.where(k_lane < counts[t], 0.0, -1e30) for t in range(2)]

    for peer in groups:
        notes.go(dest, dall.at[note], peer)
    for dz in range(2):
        for dc in range(2):
            if dz or dc:
                biases.go(bias1, ball.at[zl * 2 + c], at(x, y, (zl + dz) % 2, (c + dc) % 2, m))
    f2p[mine] = fc2[:, pl.ds(pl.multiple_of(mine * 128, 128), 128)]
    dall[note] = dest[...]
    ball[zl * 2 + c] = bias1[...]
    wout_all[z, c] = wout[half_rows, :]
    loads[2].wait()

    gain1 = attn_gain[...].reshape(1, 1280).astype(F32)

    def norm_rows(i, carry):
        r = pl.ds(pl.multiple_of(i * 32, 32), 32)
        xn[r, :] = normed(patches[r, :].astype(F32), gain1).astype(BF)
        return carry

    lax.fori_loop(0, 16, norm_rows, 0)

    hop0(1)
    early(3, 5)
    lane = lax.broadcasted_iota(jnp.int32, (256, 320), 1)
    for t in range(2):
        xt = xn[256 * t : 256 * (t + 1), :]
        q, k, v = (dot(xt, wqkv[j], NT).astype(BF) for j in range(3))
        out = jnp.zeros((256, 320), F32)
        for h in range(4):
            inside = (lane >= 80 * h) & (lane < 80 * (h + 1))
            sc = dot(jnp.where(inside, q, jnp.zeros_like(q)), k, NT) * HEAD_DIM ** (-0.5)
            sc = sc + key_bias[t]
            sc = jnp.exp(sc - jnp.max(sc, axis=1, keepdims=True))
            w = (sc / jnp.sum(sc, axis=1, keepdims=True)).astype(BF)
            out = jnp.where(inside, dot(w, v), out)
        att[2 * t : 2 * t + 2] = out.astype(BF).reshape(2, 128, 320)
    hop0(2)
    ms = [(m + k) % 4 for k in range(4)]
    halves = (slice(0, 64), slice(64, 128))
    via = [
        parts_by.go(att.at[ms[2], halves[k]], att_mid.at[k], across[1 + k]) for k in range(2)
    ]
    parts.go(att.at[ms[1]], attr.at[m], across[1])
    parts.go(att.at[ms[3]], attr.at[m], across[2])
    attr[m] = att[m]
    hop0(3)
    early(5, 6)
    for k in range(2):
        via[k].wait_recv()
        parts_on.go(att_mid.at[k], attr.at[ms[3 - 2 * k], halves[k]], across[1 + k])
    hop0(4)
    early(6, 8)
    finish0()
    parts.wait_recv()
    parts_on.wait_recv()
    for k in range(4):
        w = wout_all[2 * k : 2 * k + 2].reshape(320, 1280)
        part = dot(attr[k], w)
        nrm[...] = part if k == 0 else nrm[...] + part
    gain2 = merge_gain[...].reshape(1, 1280).astype(F32)
    for i in range(4):
        r = pl.ds(pl.multiple_of(m * 128 + 32 * i, 32), 32)
        o = (patches[r, :].astype(F32) + nrm[32 * i : 32 * (i + 1), :]).astype(BF)
        o = normed(o.astype(F32), gain2)
        for b in range(10):
            turn[b, 32 * i : 32 * (i + 1), :] = o[:, 128 * b : 128 * (b + 1)]
    for p in range(4):
        for b in range(10):
            cols = slice(128 * b, 128 * (b + 1))
            blk1[p, :, cols] = turn[b, pl.ds(p, 32, stride=4), :].astype(BF)

    loads[3].wait()

    @pl.when(odd_out)
    def _():
        relays[1].wait_recv()

    hop1, finish1, more = column_gather(
        wire, fc1_all.at[0:7, 0], fc1_all.at[0:4], BY_ROWS, fc1, fc1_all, pos
    )
    planes = [wire.batch(fc2_all.at[:, :, 0:15]) for _ in range(2)]
    batches += more + planes
    fc1_all[z, c] = fc1[...]

    def point(*calls):
        def run():
            for call, k in calls:
                call(k)

        return run

    pieces.wait_recv()
    hop2, finish2, more = column_gather(
        wire, fc2_all.at[0:7, 0], fc2_all.at[0:4], (slice(0, 8), slice(8, 16)), f2p, fc2_all, pos
    )
    batches += more
    fc2_all[z, c] = f2p[...]
    plane_gather(
        planes[0],
        blk1,
        rows_all,
        [
            point((hop1, 0)),
            point((hop1, 1), (drip, 0)),
            point((hop1, 2), (drip, 1)),
            point((hop1, 3), (drip, 2)),
            point((hop1, 4), (hop2, 0), (drip, 3)),
            point(),
        ],
        pos,
    )
    finish1()
    biases.wait_recv()
    for p in range(4):
        part = dot(
            fc1_all[2 * p : 2 * p + 2].reshape(320, 1280), rows_all[p].reshape(512, 1280), NT
        )
        acc1[...] = part if p == 0 else acc1[...] + part
    for b in range(4):
        h = acc1[80 * b : 80 * (b + 1), :] + ball[b][:, :1].astype(F32)
        blk2[b] = (0.5 * h * (1.0 + lax.erf(h * 0.5**0.5))).astype(BF)

    plane_gather(
        planes[1],
        blk2,
        hid_all,
        [
            point(),
            point((hop2, 1), (drip, 4)),
            point((hop2, 2), (drip, 5)),
            point((hop2, 3), (drip, 6)),
            point((hop2, 4), (drip, 7)),
            point(),
        ],
        pos,
    )
    finish2()

    direct = wire.batch(emb.at[0:2], shared=True)
    halfway = wire.batch(emb.at[0])
    onward = wire.batch(emb.at[0], shared=True)
    picked = wire.batch(got.at[0:63], shared=True)
    sums = wire.batch(sq_all.at[0:3], shared=True)
    batches += [direct, halfway, onward, picked, sums]
    ms = [(m + k) % 4 for k in range(4)]
    upper, lower = slice(0, 256), slice(256, 512)
    via = []
    for half in range(2):
        r = (upper, lower)[half]
        for b in range(4):
            w = jnp.concatenate(
                [fc2_all[2 * k + b // 2, b % 2].reshape(1280, 128) for k in range(4)], axis=1
            )
            part = dot(hid_all[b, :, :, :, r].reshape(1280, 256), w, TN)
            acc[...] = part if b == 0 else acc[...] + part
        for k in range(4):
            second[k, r, :] = acc[:, 128 * k : 128 * (k + 1)].astype(BF)
        via.append(halfway.go(second.at[ms[2], r], mid.at[half], across[1 + half]))
        for k in (1, 3):
            direct.go(second.at[ms[k], r], emb.at[m, r], across[1 + k // 2])
    emb[m] = second[m]
    for half in range(2):
        via[half].wait_recv()
        r = (upper, lower)[half]
        onward.go(mid.at[half], emb.at[ms[3 - 2 * half], r], across[1 + half])
    notes.wait_recv()
    near = dall[pl.ds(pl.multiple_of((zl * 2 + c) * 16, 16), 16)]
    receiver = lax.broadcasted_iota(jnp.int32, (64, 128), 0)
    odd = lax.broadcasted_iota(jnp.int32, (64, 128), 1) % 2
    bias2 = fc2_bias[...].reshape(1, 2048).astype(F32)
    own_bias = jnp.zeros((1, 128), F32)
    for b in range(16):
        own_bias = jnp.where(mine == b, bias2[:, 128 * b : 128 * (b + 1)], own_bias)
    direct.wait_recv()
    onward.wait_recv()
    for q in range(16):
        e = emb[:, 32 * q : 32 * (q + 1), :].reshape(128, 128)
        e = (e.astype(F32) + own_bias).astype(BF)
        to_here = receiver == near[q] // 512
        for i in range(2):
            pick = (to_here & (odd == i)).astype(F32).astype(BF)
            flat[pl.ds(2 * q + i, 64, stride=32), :] = dot(pick, e)
    send_rows[...] = flat[...].astype(BF).reshape(64, 32, 128)
    for peer in groups:
        picked.go(send_rows.at[peer[0] * 4 + peer[1]], got.at[s * 4 + x], peer)
    got[s * 4 + x] = send_rows[s * 4 + x]
    d = dall[...].reshape(64, 128)
    low = (s * 4 + x) * 512
    row = lax.broadcasted_iota(jnp.int32, (64, 512), 1)
    here = (d >= low) & (d < low + 512)
    puts = []
    for i in range(2):
        spot = jnp.max(jnp.where(here & (odd == i), (d - low).astype(F32), -1.0), axis=1, keepdims=True)
        puts.append((row == spot.astype(jnp.int32)).astype(F32).astype(BF))
    loads[4].wait()

    @pl.when(c == 1)
    def _():
        relays[0].wait_recv()

    @pl.when((c == 0) & (s > 0))
    def _():
        all_in.wait_recv()

    picked.wait_recv()
    flat[...] = got[...].reshape(2048, 128).astype(F32)
    ones = jnp.ones((64, 128), BF)
    first = s == 0
    squares = [jnp.zeros((128, 128), F32) for _ in range(4)]
    hits = [
        dot(puts[0][:, 128 * r : 128 * (r + 1)], ones, TN)
        + dot(puts[1][:, 128 * r : 128 * (r + 1)], ones, TN)
        for r in range(4)
    ]
    for b in range(16):
        new = [
            jnp.concatenate(
                [
                    flat[pl.ds(((b // 4 * 4 + zc) * 4 + b % 4) * 32 + i, 16, stride=2), :]
                    for zc in range(4)
                ],
                axis=0,
            ).astype(BF)
            for i in range(2)
        ]
        cols = slice(128 * b, 128 * (b + 1))
        for r in range(4):
            rr = slice(128 * r, 128 * (r + 1))
            placed = dot(puts[0][:, rr], new[0], TN) + dot(puts[1][:, rr], new[1], TN)
            seq = jnp.where(hits[r] > 0.5, placed, text[rr, cols].astype(F32))
            seq_out[rr, cols] = seq.astype(BF)
            enter = jnp.where(first, seq, incoming[rr, cols].astype(F32))
            squares[r] = squares[r] + enter * enter
    sub = lax.broadcasted_iota(jnp.int32, (8, 128), 0)
    total = jnp.zeros((8, 128), F32)
    for r in range(4):
        line = jnp.broadcast_to(jnp.sum(squares[r], axis=1, keepdims=True), (128, 128)).T
        total = jnp.where(sub == r, line[0:8], total)
    sq_own[...] = total
    for peer in across:
        sums.go(sq_own, sq_all.at[m], peer)
    sq_all[m] = total
    sums.wait_recv()
    total = (sq_all[0] + sq_all[1]) + (sq_all[2] + sq_all[3])
    scale = lax.rsqrt(total / HID + llm_eps)
    gain3 = llm_gain[...].reshape(1, 2048).astype(F32)
    for r in range(4):
        by = jnp.broadcast_to(scale[r : r + 1, :], (128, 128)).T
        rr = slice(128 * r, 128 * (r + 1))
        for b in range(16):
            cols = slice(128 * b, 128 * (b + 1))
            enter = jnp.where(first, seq_out[rr, cols].astype(F32), incoming[rr, cols].astype(F32))
            layer_out[rr, cols] = (enter * by * gain3[:, cols]).astype(BF)
    for batch in batches:
        batch.wait_send()

    @pl.when(c == 0)
    def _():
        relays[0].wait_send()

    @pl.when((c == 1) & (zl == 1) & (y < 3))
    def _():
        relays[1].wait_send()

    @pl.when(even_out | odd_out)
    def _():
        drips_out.wait_send()

    @pl.when(early_out)
    def _():
        earlies_out.wait_send()


def per_device(
    patches, patch_counts, dest_rows, qkv_weight, out_weight, attn_gain, merge_gain,
    fc1_weight, fc1_bias, fc2_weight, fc2_bias, text_embeds, section_hidden, llm_gain,
):
    vm = pl.BlockSpec(memory_space=pltpu.VMEM)
    hbm = pl.BlockSpec(memory_space=pl.ANY)
    dma = pltpu.SemaphoreType.DMA
    return pl.pallas_call(
        step_kernel,
        out_shape=[pltpu.VMEM((512, 2048), BF)] * 2,
        in_specs=[pl.BlockSpec(memory_space=pltpu.SMEM)] + [vm] * 7 + [hbm] * 6,
        out_specs=[vm] * 2,
        scratch_shapes=[
            pltpu.VMEM((3, 320, 1280), BF),
            pltpu.VMEM((320, 1280), BF),
            pltpu.VMEM((80, 1280), BF),
            pltpu.VMEM((80, 2048), BF),
            pltpu.VMEM((1, 128), jnp.int32),
            pltpu.VMEM((80, 128), BF),
            pltpu.VMEM((512, 2048), BF),
            pltpu.VMEM((512, 2048), BF),
            pltpu.VMEM((256, 2048), BF),
            pltpu.VMEM((512, 1280), BF),
            pltpu.VMEM((4, 128, 320), BF),
            pltpu.VMEM((2, 64, 320), BF),
            pltpu.VMEM((4, 128, 320), BF),
            pltpu.VMEM((8, 2, 80, 1280), BF),
            pltpu.VMEM((16, 80, 128), BF),
            pltpu.VMEM((64, 1, 128), jnp.int32),
            pltpu.VMEM((4, 80, 128), BF),
            pltpu.VMEM((128, 1280), F32),
            pltpu.VMEM((10, 128, 128), F32),
            pltpu.VMEM((4, 32, 1280), BF),
            pltpu.VMEM((4, 4, 4, 32, 1280), BF),
            pltpu.VMEM((8, 2, 80, 1280), BF),
            pltpu.VMEM((4, 80, 512), BF),
            pltpu.VMEM((4, 4, 4, 80, 512), BF),
            pltpu.VMEM((8, 2, 16, 80, 128), BF),
            pltpu.VMEM((320, 512), F32),
            pltpu.VMEM((256, 512), F32),
            pltpu.VMEM((4, 512, 128), BF),
            pltpu.VMEM((2, 256, 128), BF),
            pltpu.VMEM((4, 512, 128), BF),
            pltpu.VMEM((2048, 128), F32),
            pltpu.VMEM((64, 32, 128), BF),
            pltpu.VMEM((64, 32, 128), BF),
            pltpu.VMEM((8, 128), F32),
            pltpu.VMEM((4, 8, 128), F32),
            dma((20,)),
            dma((3 * 15 + 80 + 13,)),
            dma((5,)),
            dma((4,)),
            dma((3,)),
        ],
        compiler_params=pltpu.CompilerParams(
            collective_id=1, has_side_effects=True, vmem_limit_bytes=54 * 2**20
        ),
    )(
        patch_counts, patches, attn_gain, merge_gain, fc1_bias, fc2_bias, dest_rows, llm_gain,
        qkv_weight.transpose(1, 2, 0), out_weight, fc1_weight.T, fc2_weight,
        text_embeds, section_hidden,
    )


def solution(mesh):
    in_specs = (
        P(("section", "dp"), None),
        P(("section", "dp")),
        P(("section", "dp")),
        P(None, None, "mp"),
        P("mp", None),
        P(),
        P(),
        P("mp", ("section", "dp")),
        P(("section", "dp")),
        P(("section", "dp"), "mp"),
        P("mp"),
        P(("section", "dp"), "mp"),
        P(("section", "dp"), "mp"),
        P("mp"),
    )
    out_specs = (P(("section", "dp"), "mp"), P(("section", "dp"), "mp"))
    return jax.shard_map(
        per_device, mesh=mesh, in_specs=in_specs, out_specs=out_specs, check_vma=False
    )
```

```python
import jax
import jax.numpy as jnp
from jax import lax
from jax.experimental import pallas as pl
from jax.experimental.pallas import tpu as pltpu
from jax.sharding import PartitionSpec as P

HEAD_DIM = 80
HID = 8192
MESH = pl.DeviceIdType.MESH
BF = jnp.bfloat16
F32 = jnp.float32

vit_eps = 1e-06
llm_eps = 1e-06


def place():
    s = lax.axis_index("section")
    x = lax.axis_index("dp")
    m = lax.axis_index("mp")
    return x, s // 4, (s // 2) % 2, s % 2, m


def at(x, y, zl, c, m):
    return (y * 4 + zl * 2 + c, x, m)


class Wire:
    def __init__(self, send, recv):
        self.send, self.recv, self.sends, self.recvs = send, recv, 0, 0

    def batch(self, sent, shared=None):
        k = self.sends
        self.sends += 1
        if shared is not None:
            shared, self.recvs = self.recvs, self.recvs + 1
        return Batch(self, k, sent, shared)


class Batch:
    def __init__(self, wire, k, sent, shared):
        self.wire, self.sem, self.sent, self.shared = wire, wire.send.at[k], sent, shared

    def describe(self, src, dst, k, peer):
        return pltpu.make_async_remote_copy(
            src_ref=src, dst_ref=dst, send_sem=self.sem, recv_sem=self.wire.recv.at[k],
            device_id=peer, device_id_type=MESH,
        )

    def go(self, src, dst, peer):
        k = self.shared
        if k is None:
            k, self.wire.recvs = self.wire.recvs, self.wire.recvs + 1
        copy = self.describe(src, dst, k, peer)
        copy.start()
        self.peer = peer
        return copy

    def wait_recv(self):
        self.describe(self.sent, self.sent, self.shared, self.peer).wait_recv()

    def wait_send(self):
        self.describe(self.sent, self.sent, 0, self.peer).wait_send()


def column_gather(wire, ring_bytes, side_bytes, halves, col, column, pos, upward=(0,)):
    x, y, zl, c, m = pos
    z = 2 * m + zl
    zs = [(z + k) % 8 for k in range(8)]

    def zdev(zz, cc):
        return at(x, y, zz % 2, cc, zz // 2)

    above, below, twin = zdev(zs[1], c), zdev(zs[7], c), zdev(z, 1 - c)
    up, down = {}, {}
    up_far, down_far = upward, tuple(j for j in range(2) if j not in upward)
    ring, side = wire.batch(ring_bytes), wire.batch(side_bytes, shared=True)

    def hop(k):
        if k == 0:
            for j in range(2):
                src, dst = col.at[halves[j]], column.at[z, c].at[halves[j]]
                up[1, j] = ring.go(src, dst, above)
                down[1, j] = ring.go(src, dst, below)
            side.go(col, column.at[z, c], twin)
            return
        for j in range(2):
            for ways, z_from, peer, far in ((up, zs[8 - k], above, up_far), (down, zs[k], below, down_far)):
                if k < 4 or j in far:
                    ways[k, j].wait_recv()
                if k < 3 or (k == 3 and j in far):
                    ref = column.at[z_from, c].at[halves[j]]
                    ways[k + 1, j] = ring.go(ref, ref, peer)
        for z_from in [zs[8 - k], zs[k]][: 2 if k < 4 else 1]:
            ref = column.at[z_from, c]
            side.go(ref, ref, twin)

    return hop, side.wait_recv, [ring, side]


def shared_gather(wire, col, column, half_bytes, side_bytes, pos):
    x, y, zl, c, m = pos
    z = 2 * m + zl
    zs = [(z + k) % 8 for k in range(8)]

    def zdev(zz, cc):
        return at(x, y, zz % 2, cc, zz // 2)

    above, below, twin = zdev(zs[1], c), zdev(zs[7], c), zdev(z, 1 - c)
    right, left = at((x + 1) % 4, y, zl, c, m), at((x + 3) % 4, y, zl, c, m)
    mine = pl.ds(pl.multiple_of((x % 2) * 640, 128), 640)
    other = pl.ds(pl.multiple_of((1 - x % 2) * 640, 128), 640)
    ring, across = wire.batch(half_bytes), wire.batch(half_bytes)
    side = wire.batch(side_bytes, shared=True)
    ways = {}
    crossed = []

    def hop(k):
        if k == 0:
            dst = column.at[z, c].at[:, mine]
            ways["up", 1] = ring.go(col.at[:, mine], dst, above)
            ways["down", 1] = ring.go(col.at[:, mine], dst, below)
            side.go(col, column.at[z, c], twin)
            return
        for way, z_from, peer, beside, end in (
            ("up", zs[8 - k], above, right, 4), ("down", zs[k], below, left, 3)
        ):
            if k <= end:
                ways[way, k].wait_recv()
                ref = column.at[z_from, c].at[:, mine]
                if k < end:
                    ways[way, k + 1] = ring.go(ref, ref, peer)
                crossed.append((across.go(ref, ref, beside), column.at[z_from, c].at[:, other]))
                side.go(ref, ref, twin)

    def finish():
        for copy, ref in crossed:
            copy.wait_recv()
            side.go(ref, ref, twin)
        side.wait_recv()

    return hop, finish, [ring, across, side]


def plane_gather(cp, blk, plane, points, pos):
    x, y, zl, c, m = pos
    xs = [(x + k) % 4 for k in range(4)]
    ys = [(y + k) % 4 for k in range(4)]
    right, left = at(xs[1], y, zl, c, m), at(xs[3], y, zl, c, m)
    up, down = at(x, ys[1], zl, c, m), at(x, ys[3], zl, c, m)
    ahead = [[(right, left), (up, down)], [(up, down), (right, left)]]

    def block(v, a, b, lo, hi):
        fx, fy = (xs[a], ys[b]) if v == 0 else (xs[b], ys[a])
        return plane.at[2 * v + lo : 2 * v + hi, fy, fx]

    def push(v, axis, sgn, a, b, lo=0, hi=2, own=False):
        src = blk.at[2 * v + lo : 2 * v + hi] if own else block(v, a, b, lo, hi)
        return cp.go(src, block(v, a, b, lo, hi), ahead[v][axis][0 if sgn > 0 else 1])

    one, two, three, four = {}, {}, {}, {}
    for v in range(2):
        for g in (1, -1):
            one[v, g] = push(v, 0, g, 0, 0, own=True)
    for v in range(2):
        for g in (1, -1):
            three[v, 0, g] = push(v, 1, g, 0, 0, own=True)
    points[0]()
    plane[:, y, x] = blk[...]
    for g in (1, -1):
        for v in range(2):
            one[v, g].wait_recv()
            a = -g % 4
            two[v, g] = push(v, 0, g, a, 0, *((0, 1) if g > 0 else (1, 2)))
            for h in (1, -1):
                three[v, a, h] = push(v, 1, h, a, 0)
    points[1]()

    def opposite(a, between=None):
        for g in (1, -1):
            for v in range(2):
                three[v, a, g].wait_recv()
                four[v, a, g] = push(v, 1, g, a, -g % 4, *((0, 1) if g > 0 else (1, 2)))
            if between is not None and g == 1:
                between()

    opposite(0, points[2])
    for v in range(2):
        for g in (1, -1):
            two[v, g].wait_recv()
        for h in (1, -1):
            three[v, 2, h] = push(v, 1, h, 2, 0)
    points[3]()
    opposite(3)
    opposite(1)
    points[4]()
    opposite(2)
    points[5]()
    for copy in four.values():
        copy.wait_recv()


BY_ROWS = (slice(0, 48), slice(48, 80))
NT = (((1,), (1,)), ((), ()))
TN = (((0,), (0,)), ((), ()))


def dot(a, b, dims=(((1,), (0,)), ((), ()))):
    return lax.dot_general(a, b, dims, preferred_element_type=F32)


def normed(v, gain):
    v = v - jnp.mean(v, axis=-1, keepdims=True)
    return v * lax.rsqrt(jnp.mean(v * v, axis=-1, keepdims=True) + vit_eps) * gain


def step_kernel(
    counts, patches, attn_gain, merge_gain, fc1_bias, fc2_bias, dest_rows, llm_gain,
    wqkv_hbm, wout_hbm, fc1_hbm, fc2_hbm, text_hbm, hidden_hbm,
    seq_out, layer_out,
    wqkv, wout, fc1, fc2, dest, bias1,
    text, incoming, stage,
    xn, att, att_mid, attr, wout_all, f2p, dall, ball, nrm, turn, blk1, rows_all, fc1_all,
    blk2, hid_all, fc2_all, acc1, acc, second, mid, emb, flat, send_rows, got, sq_own, sq_all,
    send, recv, local, relay_send, relay_recv,
):
    pos = place()
    x, y, zl, c, m = pos
    s = y * 4 + zl * 2 + c
    z = 2 * m + zl
    mine = y * 4 + x
    note = (zl * 2 + c) * 16 + mine
    across = [(s, x, (m + k) % 4) for k in (2, 1, 3)]
    groups = [((s + i) % 16, (x + j) % 4, m) for i in range(16) for j in range(4) if i or j]
    barrier = pltpu.get_barrier_semaphore()
    column = [at(x, y, 1 - zl, c, (m + 1) % 4), at(x, y, 1 - zl, c, (m + 3) % 4)]
    peers = across + groups + column
    for peer in peers:
        pl.semaphore_signal(barrier, inc=1, device_id=peer, device_id_type=MESH)

    loads = [
        pltpu.make_async_copy(a, b, local.at[k])
        for k, (a, b) in enumerate(
            ((wout_hbm, wout), (fc2_hbm, fc2), (wqkv_hbm, wqkv), (fc1_hbm, fc1), (text_hbm, text))
        )
    ]
    for copy in loads:
        copy.start()

    pl.semaphore_wait(barrier, len(peers))

    wire = Wire(send, recv)
    relay_to = [at(x, y, zl, 1, m), at(x, (y + 1) % 4, 1, 0, m), at(x, y, 1 - zl, 0, m)]
    relays = [
        pltpu.make_async_remote_copy(
            src_ref=src, dst_ref=ref, send_sem=relay_send.at[k], recv_sem=relay_recv.at[k],
            device_id=relay_to[k], device_id_type=MESH,
        )
        for k, src, ref in ((0, hidden_hbm, incoming), (1, hidden_hbm.at[192:512], stage))
    ]
    early_out = (c == 1) & (s < 15)
    earlies = [
        pltpu.make_async_remote_copy(
            src_ref=hidden_hbm.at[32 * k : 32 * (k + 1)],
            dst_ref=incoming.at[32 * k : 32 * (k + 1)],
            send_sem=relay_send.at[3], recv_sem=relay_recv.at[2],
            device_id=((s + 1) % 16, x, m), device_id_type=MESH,
        )
        for k in range(6)
    ]

    def early(lo, hi):
        @pl.when(early_out)
        def _():
            for k in range(lo, hi):
                earlies[k].start()

    even_out, odd_out = (c == 1) & (zl == 0), (c == 0) & (zl == 1) & (y > 0)
    drips = []
    for k in range(10):
        r, r_stage = (slice(32 * k + low, 32 * (k + 1) + low) for low in (192, 0))
        drips.append(
            [
                pltpu.make_async_remote_copy(
                    src_ref=ref, dst_ref=incoming.at[r],
                    send_sem=relay_send.at[2], recv_sem=relay_recv.at[2],
                    device_id=relay_to[2], device_id_type=MESH,
                )
                for ref in (hidden_hbm.at[r], stage.at[r_stage])
            ]
        )
    all_in = pltpu.make_async_remote_copy(
        src_ref=incoming, dst_ref=incoming, send_sem=relay_send.at[2], recv_sem=relay_recv.at[2],
        device_id=relay_to[2], device_id_type=MESH,
    )
    drips_out, earlies_out = (
        pltpu.make_async_remote_copy(
            src_ref=ref, dst_ref=ref, send_sem=relay_send.at[k], recv_sem=relay_recv.at[2],
            device_id=relay_to[2], device_id_type=MESH,
        )
        for k, ref in ((2, stage), (3, incoming.at[0:192]))
    )

    def drip(k):
        for j in range((0, 2, 4, 6, 7, 8, 9, 10)[k], (2, 4, 6, 7, 8, 9, 10, 10)[k]):

            @pl.when(even_out)
            def _():
                drips[j][0].start()

            @pl.when(odd_out)
            def _():
                drips[j][1].start()

    loads[0].wait()
    half_rows = pl.ds(pl.multiple_of((zl * 2 + c) * 80, 16), 80)
    hop0, finish0, batches = shared_gather(
        wire, wout.at[half_rows], wout_all, fc1_all.at[0:7, 0, :, 0:640], fc1_all.at[0:4], pos
    )
    hop0(0)

    @pl.when((c == 1) & (zl == 1) & (y < 3))
    def _():
        relays[1].start()

    @pl.when(c == 0)
    def _():
        relays[0].start()

    early(0, 3)

    loads[1].wait()
    pieces = wire.batch(f2p.at[0:15], shared=True)
    notes = wire.batch(dall.at[0:63], shared=True)
    biases = wire.batch(ball.at[0:3], shared=True)
    parts = wire.batch(attr.at[0:2], shared=True)
    parts_by, parts_on = wire.batch(attr.at[0]), wire.batch(attr.at[0], shared=True)
    batches += [pieces, notes, biases, parts, parts_by, parts_on]
    for dy in range(4):
        for dx in range(4):
            if dx or dy:
                px, py = (x + dx) % 4, (y + dy) % 4
                cols = pl.ds(pl.multiple_of((py * 4 + px) * 128, 128), 128)
                pieces.go(fc2.at[:, cols], f2p.at[mine], at(px, py, zl, c, m))
    j_lane = lax.broadcasted_iota(jnp.int32, (1, 128), 1)
    dest_row = dest_rows[...].reshape(1, 128)
    tile_count = jnp.where(j_lane < 64, counts[0], counts[1])
    live = (j_lane % 64) * 4 < tile_count
    dest[...] = jnp.where(live, dest_row, 2**30)
    bias_row = fc1_bias[...].reshape(1, 80)
    top = lax.broadcasted_iota(jnp.int32, (8, 80), 0) == 0
    bias_row = jnp.where(top, bias_row.astype(F32), 0.0).astype(BF)
    bias1[...] = dot(bias_row, jnp.ones((8, 128), BF), TN).astype(BF)
    k_lane = lax.broadcasted_iota(jnp.int32, (1, 256), 1)
    key_bias = [jnp.where(k_lane < counts[t], 0.0, -1e30) for t in range(2)]

    for peer in groups:
        notes.go(dest, dall.at[note], peer)
    for dz in range(2):
        for dc in range(2):
            if dz or dc:
                biases.go(bias1, ball.at[zl * 2 + c], at(x, y, (zl + dz) % 2, (c + dc) % 2, m))
    f2p[mine] = fc2[:, pl.ds(pl.multiple_of(mine * 128, 128), 128)]
    dall[note] = dest[...]
    ball[zl * 2 + c] = bias1[...]
    wout_all[z, c] = wout[half_rows, :]
    loads[2].wait()

    gain1 = attn_gain[...].reshape(1, 1280).astype(F32)

    def norm_rows(i, carry):
        r = pl.ds(pl.multiple_of(i * 32, 32), 32)
        xn[r, :] = normed(patches[r, :].astype(F32), gain1).astype(BF)
        return carry

    lax.fori_loop(0, 16, norm_rows, 0)

    hop0(1)
    early(3, 5)
    lane = lax.broadcasted_iota(jnp.int32, (256, 320), 1)
    for t in range(2):
        xt = xn[256 * t : 256 * (t + 1), :]
        q, k, v = (dot(xt, wqkv[j], NT).astype(BF) for j in range(3))
        out = jnp.zeros((256, 320), F32)
        for h in range(4):
            inside = (lane >= 80 * h) & (lane < 80 * (h + 1))
            sc = dot(jnp.where(inside, q, jnp.zeros_like(q)), k, NT) * HEAD_DIM ** (-0.5)
            sc = sc + key_bias[t]
            sc = jnp.exp(sc - jnp.max(sc, axis=1, keepdims=True))
            w = (sc / jnp.sum(sc, axis=1, keepdims=True)).astype(BF)
            out = jnp.where(inside, dot(w, v), out)
        att[2 * t : 2 * t + 2] = out.astype(BF).reshape(2, 128, 320)
    hop0(2)
    ms = [(m + k) % 4 for k in range(4)]
    halves = (slice(0, 64), slice(64, 128))
    via = [
        parts_by.go(att.at[ms[2], halves[k]], att_mid.at[k], across[1 + k]) for k in range(2)
    ]
    parts.go(att.at[ms[1]], attr.at[m], across[1])
    parts.go(att.at[ms[3]], attr.at[m], across[2])
    attr[m] = att[m]
    hop0(3)
    early(5, 6)
    for k in range(2):
        via[k].wait_recv()
        parts_on.go(att_mid.at[k], attr.at[ms[3 - 2 * k], halves[k]], across[1 + k])
    hop0(4)
    finish0()
    parts.wait_recv()
    parts_on.wait_recv()
    for k in range(4):
        w = wout_all[2 * k : 2 * k + 2].reshape(320, 1280)
        part = dot(attr[k], w)
        nrm[...] = part if k == 0 else nrm[...] + part
    gain2 = merge_gain[...].reshape(1, 1280).astype(F32)
    for i in range(4):
        r = pl.ds(pl.multiple_of(m * 128 + 32 * i, 32), 32)
        o = (patches[r, :].astype(F32) + nrm[32 * i : 32 * (i + 1), :]).astype(BF)
        o = normed(o.astype(F32), gain2)
        for b in range(10):
            turn[b, 32 * i : 32 * (i + 1), :] = o[:, 128 * b : 128 * (b + 1)]
    for p in range(4):
        for b in range(10):
            cols = slice(128 * b, 128 * (b + 1))
            blk1[p, :, cols] = turn[b, pl.ds(p, 32, stride=4), :].astype(BF)

    loads[3].wait()

    @pl.when(odd_out)
    def _():
        relays[1].wait_recv()

    hop1, finish1, more = column_gather(
        wire, fc1_all.at[0:7, 0], fc1_all.at[0:4], BY_ROWS, fc1, fc1_all, pos
    )
    planes = [wire.batch(fc2_all.at[:, :, 0:15]) for _ in range(2)]
    batches += more + planes
    fc1_all[z, c] = fc1[...]

    def point(*calls):
        def run():
            for call, k in calls:
                call(k)

        return run

    pieces.wait_recv()
    hop2, finish2, more = column_gather(
        wire, fc2_all.at[0:7, 0], fc2_all.at[0:4], (slice(0, 8), slice(8, 16)), f2p, fc2_all, pos
    )
    batches += more
    fc2_all[z, c] = f2p[...]
    plane_gather(
        planes[0],
        blk1,
        rows_all,
        [
            point((hop1, 0)),
            point((hop1, 1), (drip, 0)),
            point((hop1, 2), (drip, 1)),
            point((hop1, 3), (drip, 2)),
            point((hop1, 4), (hop2, 0), (drip, 3)),
            point(),
        ],
        pos,
    )
    finish1()
    biases.wait_recv()
    for p in range(4):
        part = dot(
            fc1_all[2 * p : 2 * p + 2].reshape(320, 1280), rows_all[p].reshape(512, 1280), NT
        )
        acc1[...] = part if p == 0 else acc1[...] + part
    for b in range(4):
        h = acc1[80 * b : 80 * (b + 1), :] + ball[b][:, :1].astype(F32)
        blk2[b] = (0.5 * h * (1.0 + lax.erf(h * 0.5**0.5))).astype(BF)

    plane_gather(
        planes[1],
        blk2,
        hid_all,
        [
            point(),
            point((hop2, 1), (drip, 4)),
            point((hop2, 2), (drip, 5)),
            point((hop2, 3), (drip, 6)),
            point((hop2, 4), (drip, 7)),
            point(),
        ],
        pos,
    )
    finish2()

    direct = wire.batch(emb.at[0:2], shared=True)
    halfway = wire.batch(emb.at[0])
    onward = wire.batch(emb.at[0], shared=True)
    picked = wire.batch(got.at[0:63], shared=True)
    sums = wire.batch(sq_all.at[0:3], shared=True)
    batches += [direct, halfway, onward, picked, sums]
    ms = [(m + k) % 4 for k in range(4)]
    upper, lower = slice(0, 256), slice(256, 512)
    via = []
    for half in range(2):
        r = (upper, lower)[half]
        for b in range(4):
            w = jnp.concatenate(
                [fc2_all[2 * k + b // 2, b % 2].reshape(1280, 128) for k in range(4)], axis=1
            )
            part = dot(hid_all[b, :, :, :, r].reshape(1280, 256), w, TN)
            acc[...] = part if b == 0 else acc[...] + part
        for k in range(4):
            second[k, r, :] = acc[:, 128 * k : 128 * (k + 1)].astype(BF)
        via.append(halfway.go(second.at[ms[2], r], mid.at[half], across[1 + half]))
        for k in (1, 3):
            direct.go(second.at[ms[k], r], emb.at[m, r], across[1 + k // 2])
    emb[m] = second[m]
    for half in range(2):
        via[half].wait_recv()
        r = (upper, lower)[half]
        onward.go(mid.at[half], emb.at[ms[3 - 2 * half], r], across[1 + half])
    notes.wait_recv()
    near = dall[pl.ds(pl.multiple_of((zl * 2 + c) * 16, 16), 16)]
    receiver = lax.broadcasted_iota(jnp.int32, (64, 128), 0)
    odd = lax.broadcasted_iota(jnp.int32, (64, 128), 1) % 2
    bias2 = fc2_bias[...].reshape(1, 2048).astype(F32)
    own_bias = jnp.zeros((1, 128), F32)
    for b in range(16):
        own_bias = jnp.where(mine == b, bias2[:, 128 * b : 128 * (b + 1)], own_bias)
    direct.wait_recv()
    onward.wait_recv()
    for q in range(16):
        e = emb[:, 32 * q : 32 * (q + 1), :].reshape(128, 128)
        e = (e.astype(F32) + own_bias).astype(BF)
        to_here = receiver == near[q] // 512
        for i in range(2):
            pick = (to_here & (odd == i)).astype(F32).astype(BF)
            flat[pl.ds(2 * q + i, 64, stride=32), :] = dot(pick, e)
    send_rows[...] = flat[...].astype(BF).reshape(64, 32, 128)
    for peer in groups:
        picked.go(send_rows.at[peer[0] * 4 + peer[1]], got.at[s * 4 + x], peer)
    got[s * 4 + x] = send_rows[s * 4 + x]
    d = dall[...].reshape(64, 128)
    low = (s * 4 + x) * 512
    row = lax.broadcasted_iota(jnp.int32, (64, 512), 1)
    here = (d >= low) & (d < low + 512)
    puts = []
    for i in range(2):
        spot = jnp.max(jnp.where(here & (odd == i), (d - low).astype(F32), -1.0), axis=1, keepdims=True)
        puts.append((row == spot.astype(jnp.int32)).astype(F32).astype(BF))
    loads[4].wait()

    @pl.when(c == 1)
    def _():
        relays[0].wait_recv()

    @pl.when((c == 0) & (s > 0))
    def _():
        all_in.wait_recv()

    picked.wait_recv()
    flat[...] = got[...].reshape(2048, 128).astype(F32)
    ones = jnp.ones((64, 128), BF)
    first = s == 0
    squares = [jnp.zeros((128, 128), F32) for _ in range(4)]
    hits = [
        dot(puts[0][:, 128 * r : 128 * (r + 1)], ones, TN)
        + dot(puts[1][:, 128 * r : 128 * (r + 1)], ones, TN)
        for r in range(4)
    ]
    for b in range(16):
        new = [
            jnp.concatenate(
                [
                    flat[pl.ds(((b // 4 * 4 + zc) * 4 + b % 4) * 32 + i, 16, stride=2), :]
                    for zc in range(4)
                ],
                axis=0,
            ).astype(BF)
            for i in range(2)
        ]
        cols = slice(128 * b, 128 * (b + 1))
        for r in range(4):
            rr = slice(128 * r, 128 * (r + 1))
            placed = dot(puts[0][:, rr], new[0], TN) + dot(puts[1][:, rr], new[1], TN)
            seq = jnp.where(hits[r] > 0.5, placed, text[rr, cols].astype(F32))
            seq_out[rr, cols] = seq.astype(BF)
            enter = jnp.where(first, seq, incoming[rr, cols].astype(F32))
            squares[r] = squares[r] + enter * enter
    sub = lax.broadcasted_iota(jnp.int32, (8, 128), 0)
    total = jnp.zeros((8, 128), F32)
    for r in range(4):
        line = jnp.broadcast_to(jnp.sum(squares[r], axis=1, keepdims=True), (128, 128)).T
        total = jnp.where(sub == r, line[0:8], total)
    sq_own[...] = total
    for peer in across:
        sums.go(sq_own, sq_all.at[m], peer)
    sq_all[m] = total
    sums.wait_recv()
    total = (sq_all[0] + sq_all[1]) + (sq_all[2] + sq_all[3])
    scale = lax.rsqrt(total / HID + llm_eps)
    gain3 = llm_gain[...].reshape(1, 2048).astype(F32)
    for r in range(4):
        by = jnp.broadcast_to(scale[r : r + 1, :], (128, 128)).T
        rr = slice(128 * r, 128 * (r + 1))
        for b in range(16):
            cols = slice(128 * b, 128 * (b + 1))
            enter = jnp.where(first, seq_out[rr, cols].astype(F32), incoming[rr, cols].astype(F32))
            layer_out[rr, cols] = (enter * by * gain3[:, cols]).astype(BF)
    for batch in batches:
        batch.wait_send()

    @pl.when(c == 0)
    def _():
        relays[0].wait_send()

    @pl.when((c == 1) & (zl == 1) & (y < 3))
    def _():
        relays[1].wait_send()

    @pl.when(even_out | odd_out)
    def _():
        drips_out.wait_send()

    @pl.when(early_out)
    def _():
        earlies_out.wait_send()


def per_device(
    patches, patch_counts, dest_rows, qkv_weight, out_weight, attn_gain, merge_gain,
    fc1_weight, fc1_bias, fc2_weight, fc2_bias, text_embeds, section_hidden, llm_gain,
):
    vm = pl.BlockSpec(memory_space=pltpu.VMEM)
    hbm = pl.BlockSpec(memory_space=pl.ANY)
    dma = pltpu.SemaphoreType.DMA
    return pl.pallas_call(
        step_kernel,
        out_shape=[pltpu.VMEM((512, 2048), BF)] * 2,
        in_specs=[pl.BlockSpec(memory_space=pltpu.SMEM)] + [vm] * 7 + [hbm] * 6,
        out_specs=[vm] * 2,
        scratch_shapes=[
            pltpu.VMEM((3, 320, 1280), BF),
            pltpu.VMEM((320, 1280), BF),
            pltpu.VMEM((80, 1280), BF),
            pltpu.VMEM((80, 2048), BF),
            pltpu.VMEM((1, 128), jnp.int32),
            pltpu.VMEM((80, 128), BF),
            pltpu.VMEM((512, 2048), BF),
            pltpu.VMEM((512, 2048), BF),
            pltpu.VMEM((320, 2048), BF),
            pltpu.VMEM((512, 1280), BF),
            pltpu.VMEM((4, 128, 320), BF),
            pltpu.VMEM((2, 64, 320), BF),
            pltpu.VMEM((4, 128, 320), BF),
            pltpu.VMEM((8, 2, 80, 1280), BF),
            pltpu.VMEM((16, 80, 128), BF),
            pltpu.VMEM((64, 1, 128), jnp.int32),
            pltpu.VMEM((4, 80, 128), BF),
            pltpu.VMEM((128, 1280), F32),
            pltpu.VMEM((10, 128, 128), F32),
            pltpu.VMEM((4, 32, 1280), BF),
            pltpu.VMEM((4, 4, 4, 32, 1280), BF),
            pltpu.VMEM((8, 2, 80, 1280), BF),
            pltpu.VMEM((4, 80, 512), BF),
            pltpu.VMEM((4, 4, 4, 80, 512), BF),
            pltpu.VMEM((8, 2, 16, 80, 128), BF),
            pltpu.VMEM((320, 512), F32),
            pltpu.VMEM((256, 512), F32),
            pltpu.VMEM((4, 512, 128), BF),
            pltpu.VMEM((2, 256, 128), BF),
            pltpu.VMEM((4, 512, 128), BF),
            pltpu.VMEM((2048, 128), F32),
            pltpu.VMEM((64, 32, 128), BF),
            pltpu.VMEM((64, 32, 128), BF),
            pltpu.VMEM((8, 128), F32),
            pltpu.VMEM((4, 8, 128), F32),
            dma((20,)),
            dma((3 * 15 + 80 + 13,)),
            dma((5,)),
            dma((4,)),
            dma((3,)),
        ],
        compiler_params=pltpu.CompilerParams(
            collective_id=1, has_side_effects=True, vmem_limit_bytes=54 * 2**20
        ),
    )(
        patch_counts, patches, attn_gain, merge_gain, fc1_bias, fc2_bias, dest_rows, llm_gain,
        qkv_weight.transpose(1, 2, 0), out_weight, fc1_weight.T, fc2_weight,
        text_embeds, section_hidden,
    )


def solution(mesh):
    in_specs = (
        P(("section", "dp"), None),
        P(("section", "dp")),
        P(("section", "dp")),
        P(None, None, "mp"),
        P("mp", None),
        P(),
        P(),
        P("mp", ("section", "dp")),
        P(("section", "dp")),
        P(("section", "dp"), "mp"),
        P("mp"),
        P(("section", "dp"), "mp"),
        P(("section", "dp"), "mp"),
        P("mp"),
    )
    out_specs = (P(("section", "dp"), "mp"), P(("section", "dp"), "mp"))
    return jax.shard_map(
        per_device, mesh=mesh, in_specs=in_specs, out_specs=out_specs, check_vma=False
    )
```
